32 devices in a mesh: row: 8 (over y, x, core), col: 4 (over z).
Axes of the slice: x: 2, y: 2, z: 4, core: 2. Of those that a mesh axis runs over, the one named last changes fastest.
Arguments:
- points_here: float32 [4, 3, 32, 64, 128], P(None, None, 'row', 'col'), may hold values from -4 to 4
- points_there: float32 [4, 3, 32, 64, 128], P(None, None, 'row', 'col'), may hold values from -4 to 4
- outlier_mask: int32 [4, 32, 64, 128], P(None, 'row', 'col'), may hold values 0 or 1
- transforms: float32 [3, 4, 32, 64], P(None, None, 'row', 'col'), may hold values from -3 to 3
Outputs:
- aligned: float32 [3, 4, 32, 64], P(None, None, 'row', 'col')
- error_stats: float32 [2, 2], replicated
The draws below stay inside these ranges and needn't reach their ends.
All inputs are finite; a program needn't handle non-finite values. No bound on the sum of `outlier_mask` on one device may be relied on, other than what follows from the above.
Results may differ from the reference program's by a relative error of at most 0.0003.
Values sent between devices are 32-bit elements; how exact they have to be, the bound alone decides.
No kernel may reach another device: no remote copies, remote signals or barrier semaphores. Data moves between devices by JAX's collectives and lax.ppermute only.
A program may use at most 64 MiB of HBM per device.

```python
import jax
import jax.numpy as jnp
from jax import lax

PAIRS = 128
LINKS = 4
ITERS = 2
GR = 32
GC = 64


def set_ends(array, rng, smallest, high):
    shape = array.shape
    place = [jax.random.randint(jax.random.fold_in(rng, axis), (), 0, shape[axis]) for axis in range(len(shape))]
    array = array.at[tuple(place)].set(smallest)
    longest = shape.index(max(shape))
    place[longest] = (place[longest] + 1) % shape[longest]
    return array.at[tuple(place)].set(high)


def block_levels(rng, extent, pieces, smallest, top_value):
    gain = 1.0
    for position, parts in pieces:
        heights = jax.random.uniform(jax.random.fold_in(jax.random.fold_in(rng, 6), position), (parts,), jnp.float32, smallest / len(pieces), top_value / len(pieces))
        gain = gain * jnp.repeat(jnp.exp(heights), extent[position] // parts).reshape((-1,) + (1,) * (len(extent) - 1 - position))
    return gain


def bell_draw(key, extent, deviation, limit, split=(), kind=jnp.bfloat16):
    drawn = jax.random.normal(key, extent, jnp.float32) * deviation
    if len(split) > 0:
        drawn = block_levels(key, extent, split, -0.22, 0.18) * drawn
    return jnp.clip(drawn, min=-limit, max=limit).astype(kind)


def setup_inputs(seed: int = 0) -> dict:
    streams_of = jax.random.split(jax.random.key(seed), 5)
    points_here = bell_draw(streams_of[0], (LINKS, 3, GR, GC, PAIRS), 1.0, 4.0, ((2, 8), (3, 4)), jnp.float32)
    points_there = bell_draw(streams_of[1], (LINKS, 3, GR, GC, PAIRS), 1.0, 4.0, ((2, 8), (3, 4)), jnp.float32)
    outlier_mask = set_ends((jax.random.randint(streams_of[2], (LINKS, GR, GC, PAIRS), 0, 4) < 3).astype(jnp.int32), jax.random.fold_in(streams_of[2], 1), 0, 1)
    transforms = bell_draw(streams_of[3], (3, 4, GR, GC), 0.5, 3.0, ((2, 8), (3, 4)), jnp.float32)
    return dict(points_here=points_here, points_there=points_there, outlier_mask=outlier_mask, transforms=transforms)


link_offsets = ((0, 1), (1, 0), (1, 1), (1, -1))
damping_scale = 64.0

def apply_affine(affine, points):
    mapped = []
    for component in range(3):
        value = affine[component, 3][..., None] + affine[component, 0][..., None] * points[0]
        value = value + affine[component, 1][..., None] * points[1]
        value = value + affine[component, 2][..., None] * points[2]
        mapped.append(value)
    return jnp.stack(mapped)

def link_error(here, there):
    delta = here - there
    return delta[0] * delta[0] + delta[1] * delta[1] + delta[2] * delta[2]

def gram_terms(weight, points):
    weighted = [weight * points[0], weight * points[1], weight * points[2], weight]
    entries = []
    for first in range(4):
        for second in range(4):
            if second == 3:
                entries.append(lax.optimization_barrier(jnp.sum(weighted[first], axis=-1)))
            else:
                entries.append(lax.optimization_barrier(jnp.sum(weighted[first] * points[second], axis=-1)))
    return jnp.stack(entries).reshape((4, 4) + weight.shape[:-1])

def cross_terms(weight, target, points):
    entries = []
    for component in range(3):
        scaled = weight * target[component]
        for second in range(4):
            if second == 3:
                entries.append(lax.optimization_barrier(jnp.sum(scaled, axis=-1)))
            else:
                entries.append(lax.optimization_barrier(jnp.sum(scaled * points[second], axis=-1)))
    return jnp.stack(entries).reshape((3, 4) + weight.shape[:-1])

def solve_small(gram, rhs):
    factor = [[None] * 4 for _ in range(4)]
    for first in range(4):
        for second in range(first + 1):
            value = gram[first, second]
            for inner in range(second):
                value = value - factor[first][inner] * factor[second][inner]
            if first == second:
                factor[first][first] = jnp.sqrt(value)
            else:
                factor[first][second] = value / factor[second][second]
    result = []
    for component in range(3):
        forward = []
        for first in range(4):
            value = rhs[component, first]
            for inner in range(first):
                value = value - factor[first][inner] * forward[inner]
            forward.append(value / factor[first][first])
        backward = [None] * 4
        for first in (3, 2, 1, 0):
            value = forward[first]
            for inner in range(first + 1, 4):
                value = value - factor[inner][first] * backward[inner]
            backward[first] = value / factor[first][first]
        result.append(jnp.stack(backward))
    return jnp.stack(result)

def neighbour_of(affine, row_step, col_step):
    padded = jnp.pad(affine, ((0, 0), (0, 0), (0, 1), (1, 1)))
    return padded[:, :, row_step:row_step + GR, 1 + col_step:1 + col_step + GC]

def deliver(terms, row_step, col_step):
    padded = jnp.pad(terms, ((0, 0), (0, 0), (1, 0), (1, 1)))
    return padded[:, :, 1 - row_step:1 - row_step + GR, 1 - col_step:1 - col_step + GC]

def validity(row_step, col_step):
    row_ids = jnp.arange(GR, dtype=jnp.int32)
    col_ids = jnp.arange(GC, dtype=jnp.int32)
    row_valid = row_ids + row_step < GR
    col_valid = (col_ids + col_step >= 0) & (col_ids + col_step < GC)
    return (row_valid[:, None] & col_valid[None, :]).astype(jnp.float32)

def link_state(affine, points_here, points_there, outlier_mask, direction):
    row_step, col_step = link_offsets[direction]
    weight_mask = outlier_mask[direction].astype(jnp.float32) * validity(row_step, col_step)[..., None]
    here = apply_affine(affine, points_here[direction])
    there = apply_affine(neighbour_of(affine, row_step, col_step), points_there[direction])
    return (weight_mask, here, there, link_error(here, there))

def reference(points_here, points_there, outlier_mask, transforms):
    affine = transforms
    records = []
    for iteration in range(ITERS):
        largest = jnp.zeros((), jnp.float32)
        total = jnp.zeros((), jnp.float32)
        count = jnp.zeros((), jnp.float32)
        for direction in range(4):
            weight_mask, here, there, error = link_state(affine, points_here, points_there, outlier_mask, direction)
            masked = weight_mask * error
            largest = jnp.maximum(largest, jnp.max(masked))
            total = total + jnp.sum(masked)
            count = count + jnp.sum(weight_mask)
        mean_error = total / jnp.maximum(count, 1.0)
        scale = 0.25 * largest + 1e-06
        damping = damping_scale * mean_error + 1.0
        gram = jnp.zeros((4, 4, GR, GC), jnp.float32)
        cross = jnp.zeros((3, 4, GR, GC), jnp.float32)
        for direction in range(4):
            row_step, col_step = link_offsets[direction]
            weight_mask, here, there, error = link_state(affine, points_here, points_there, outlier_mask, direction)
            weight = weight_mask / (1.0 + error / scale)
            gram = gram + gram_terms(weight, points_here[direction])
            cross = cross + cross_terms(weight, there, points_here[direction])
            gram = gram + deliver(gram_terms(weight, points_there[direction]), row_step, col_step)
            cross = cross + deliver(cross_terms(weight, here, points_there[direction]), row_step, col_step)
        identity = jnp.eye(4, dtype=jnp.float32)[:, :, None, None]
        affine = solve_small(gram + damping * identity, cross + damping * affine)
        records.append(jnp.stack([largest, mean_error]))
    return (affine, jnp.stack(records, axis=1))
```

```python
import jax
import jax.numpy as jnp
from jax import lax
from jax.sharding import PartitionSpec as P

ITERS = 2


link_offsets = ((0, 1), (1, 0), (1, 1), (1, -1))
damping_scale = 64.0


def from_behind(array, axis, by):
    peers = lax.axis_size(axis)
    pairs = [(i, i + by) for i in range(peers) if 0 <= i + by < peers]
    return lax.ppermute(array, axis, pairs)


def over_devices(largest, total, count):
    devices = lax.axis_size("row") * lax.axis_size("col")
    mine = jnp.stack([largest, total, count])
    sent = jnp.broadcast_to(jnp.pad(mine, (0, 125))[None], (devices, 128))
    got = lax.all_to_all(sent, ("row", "col"), 0, 0)
    return jnp.max(got[:, 0]), jnp.sum(got[:, 1]), jnp.sum(got[:, 2])


def with_halo(block, sides, width):
    for axis, dim in sides:
        count = lax.axis_size(axis)
        forward = [(i, i + 1) for i in range(count - 1)]
        backward = [(target, source) for source, target in forward]
        low = lax.ppermute(
            lax.slice_in_dim(block, block.shape[dim] - width, None, axis=dim), axis, forward
        )
        high = lax.ppermute(lax.slice_in_dim(block, 0, width, axis=dim), axis, backward)
        block = jnp.concatenate([low, block, high], axis=dim)
    return block


def apply_affine(affine, points):
    mapped = []
    for component in range(3):
        value = affine[component, 3][..., None] + affine[component, 0][..., None] * points[0]
        value = value + affine[component, 1][..., None] * points[1]
        value = value + affine[component, 2][..., None] * points[2]
        mapped.append(value)
    return jnp.stack(mapped)


def link_error(here, there):
    delta = here - there
    return delta[0] * delta[0] + delta[1] * delta[1] + delta[2] * delta[2]


def gram_terms(weight, points):
    weighted = [weight * points[0], weight * points[1], weight * points[2], weight]
    entries = []
    for first in range(4):
        for second in range(4):
            if second == 3:
                entries.append(jnp.sum(weighted[first], axis=-1))
            else:
                entries.append(jnp.sum(weighted[first] * points[second], axis=-1))
    return jnp.stack(entries).reshape((4, 4) + weight.shape[:-1])


def cross_terms(weight, target, points):
    entries = []
    for component in range(3):
        scaled = weight * target[component]
        for second in range(4):
            if second == 3:
                entries.append(jnp.sum(scaled, axis=-1))
            else:
                entries.append(jnp.sum(scaled * points[second], axis=-1))
    return jnp.stack(entries).reshape((3, 4) + weight.shape[:-1])


def solve_small(gram, rhs):
    factor = [[None] * 4 for _ in range(4)]
    for first in range(4):
        for second in range(first + 1):
            value = gram[first, second]
            for inner in range(second):
                value = value - factor[first][inner] * factor[second][inner]
            if first == second:
                factor[first][first] = jnp.sqrt(value)
            else:
                factor[first][second] = value / factor[second][second]
    result = []
    for component in range(3):
        forward = []
        for first in range(4):
            value = rhs[component, first]
            for inner in range(first):
                value = value - factor[first][inner] * forward[inner]
            forward.append(value / factor[first][first])
        backward = [None] * 4
        for first in (3, 2, 1, 0):
            value = forward[first]
            for inner in range(first + 1, 4):
                value = value - factor[inner][first] * backward[inner]
            backward[first] = value / factor[first][first]
        result.append(jnp.stack(backward))
    return jnp.stack(result)


def move_blocks(packages):
    east_pair = jnp.stack([packages[0], packages[2]])
    arrived_east = from_behind(east_pair[:, :, :, -1:], "col", 1)
    east_pair = jnp.concatenate([arrived_east, east_pair[:, :, :, :-1]], axis=3)
    west_one = packages[3]
    arrived_west = from_behind(west_one[:, :, :1], "col", -1)
    west_one = jnp.concatenate([west_one[:, :, 1:], arrived_west], axis=2)
    south_set = jnp.stack([packages[1], east_pair[1], west_one])
    arrived_south = from_behind(south_set[:, :, -1:], "row", 1)
    south_set = jnp.concatenate([arrived_south, south_set[:, :, :-1]], axis=2)
    return [east_pair[0], south_set[0], south_set[1], south_set[2]]


def on_device(points_here, points_there, outlier_mask, transforms):
    rows_local = transforms.shape[2]
    cols_local = transforms.shape[3]
    grid_rows = rows_local * lax.axis_size("row")
    grid_cols = cols_local * lax.axis_size("col")
    row_ids = lax.axis_index("row") * rows_local + jnp.arange(rows_local, dtype=jnp.int32)
    col_ids = lax.axis_index("col") * cols_local + jnp.arange(cols_local, dtype=jnp.int32)
    weight_masks = []
    for direction in range(4):
        row_step, col_step = link_offsets[direction]
        row_valid = row_ids + row_step < grid_rows
        col_valid = (col_ids + col_step >= 0) & (col_ids + col_step < grid_cols)
        valid = (row_valid[:, None] & col_valid[None, :]).astype(jnp.float32)
        weight_masks.append(outlier_mask[direction].astype(jnp.float32) * valid[..., None])
    affine = transforms
    records = []
    for iteration in range(ITERS):
        side_ext = with_halo(affine, (("col", 3),), 1)
        below = from_behind(side_ext[:, :, :1], "row", -1)
        extended = jnp.concatenate([side_ext, below], axis=2)
        mapped_here = []
        mapped_there = []
        errors = []
        largest_local = jnp.zeros((), jnp.float32)
        total_local = jnp.zeros((), jnp.float32)
        count_local = jnp.zeros((), jnp.float32)
        for direction in range(4):
            row_step, col_step = link_offsets[direction]
            target = extended[
                :, :, row_step : row_step + rows_local, 1 + col_step : 1 + col_step + cols_local
            ]
            here = apply_affine(affine, points_here[direction])
            there = apply_affine(target, points_there[direction])
            error = link_error(here, there)
            masked = weight_masks[direction] * error
            largest_local = jnp.maximum(largest_local, jnp.max(masked))
            total_local = total_local + jnp.sum(masked)
            count_local = count_local + jnp.sum(weight_masks[direction])
            mapped_here.append(here)
            mapped_there.append(there)
            errors.append(error)
        largest, total, count = over_devices(largest_local, total_local, count_local)
        mean_error = total / jnp.maximum(count, 1.0)
        scale = 0.25 * largest + 1e-06
        damping = damping_scale * mean_error + 1.0
        gram = jnp.zeros((4, 4, rows_local, cols_local), jnp.float32)
        cross = jnp.zeros((3, 4, rows_local, cols_local), jnp.float32)
        packages = []
        for direction in range(4):
            weight = weight_masks[direction] / (1.0 + errors[direction] / scale)
            gram = gram + gram_terms(weight, points_here[direction])
            cross = cross + cross_terms(weight, mapped_there[direction], points_here[direction])
            far_gram = gram_terms(weight, points_there[direction]).reshape(
                (16, rows_local, cols_local)
            )
            far_cross = cross_terms(
                weight, mapped_here[direction], points_there[direction]
            ).reshape((12, rows_local, cols_local))
            packages.append(jnp.concatenate([far_gram, far_cross], axis=0))
        arrived = move_blocks(packages)
        for package in arrived:
            gram = gram + package[:16].reshape((4, 4, rows_local, cols_local))
            cross = cross + package[16:].reshape((3, 4, rows_local, cols_local))
        identity = jnp.eye(4, dtype=jnp.float32)[:, :, None, None]
        affine = solve_small(gram + damping * identity, cross + damping * affine)
        records.append(jnp.stack([largest, mean_error]))
    return (affine, jnp.stack(records, axis=1))


def solution(mesh):
    return jax.shard_map(
        on_device,
        mesh=mesh,
        in_specs=(
            P(None, None, "row", "col", None),
            P(None, None, "row", "col", None),
            P(None, "row", "col", None),
            P(None, None, "row", "col"),
        ),
        out_specs=(P(None, None, "row", "col"), P()),
        check_vma=False,
    )
```

```python
import jax
import jax.numpy as jnp
from jax import lax
from jax.experimental import pallas as pl
from jax.experimental.pallas import tpu as pltpu
from jax.sharding import PartitionSpec as P

ITERS = 2
LANES = 128
SUB = 8
COMPS = 7

link_offsets = ((0, 1), (1, 0), (1, 1), (1, -1))
damping_scale = 64.0
GRAM = [(a, b) for a in range(4) for b in range(a + 1)]


def whole(count):
    return [pl.BlockSpec(memory_space=pltpu.VMEM) for _ in range(count)]


def call(body, out_shapes, scratch=(), **params):
    shapes = [jax.ShapeDtypeStruct(s, jnp.float32) for s in out_shapes]

    def run(*args):
        return pl.pallas_call(
            body,
            out_shape=shapes,
            in_specs=whole(len(args)),
            out_specs=whole(len(shapes)),
            scratch_shapes=[pltpu.VMEM(s, jnp.float32) for s in scratch],
            **params,
        )(*args)

    return run


def iota(shape, axis):
    return lax.broadcasted_iota(jnp.int32, shape, axis)


def component(refs, d, c):
    here, there, mask = refs
    if c < 3:
        return here.at[d, c]
    if c < 6:
        return there.at[d, c - 3]
    return mask.at[d]


def pack_cols(rows, cols):
    def body(here, there, outlier, transforms, mask, to_east, to_west):
        grid_rows = rows * lax.axis_size("row")
        grid_cols = cols * lax.axis_size("col")
        row0 = lax.axis_index("row") * rows
        col_ids = lax.axis_index("col") * cols + iota((cols, LANES), 0)
        for d, (dr, dc) in enumerate(link_offsets):
            col_valid = jnp.where((col_ids + dc >= 0) & (col_ids + dc < grid_cols), 1.0, 0.0)
            for r in range(rows):
                row_valid = jnp.where(row0 + r + dr < grid_rows, 1.0, 0.0)
                mask[d, r] = outlier[d, r].astype(jnp.float32) * (col_valid * row_valid)
        refs = (here, there, mask)
        for d in range(4):
            for c in range(COMPS):
                src = component(refs, d, c)
                for r in range(rows):
                    at = ((d * COMPS + c) * rows + r) * 2
                    to_east[at : at + 2] = src[r, cols - 2 : cols]
                    to_west[at : at + 2] = src[r, 0:2]
        at = 4 * COMPS * rows * 2
        for out in (to_east, to_west):
            out[at:] = jnp.zeros((12 * rows, LANES), jnp.float32)
            out[at:, 0:cols] = transforms[...]

    count = 4 * COMPS * rows * 2 + 12 * rows
    return call(body, [(4, rows, cols, LANES), (count, LANES), (count, LANES)])


def pack_rows(rows, cols):
    span = cols + 4

    def body(here, there, mask, transforms, west, east, text, up_t, down, up):
        at = 4 * COMPS * rows * 2
        lane = iota((12 * rows, LANES), 1)
        text[...] = jnp.zeros((12 * rows, LANES), jnp.float32)
        text[:, 0:cols] = transforms[...]
        wide = pltpu.roll(text[...], 2, 1)
        left = pltpu.roll(west[at:], LANES - (cols - 2), 1)
        right = pltpu.roll(east[at:], cols + 2, 1)
        value = jnp.where(lane < 2, left, jnp.where(lane < cols + 2, wide, right))
        text[...] = jnp.where(lane < span, value, 0.0)
        refs = (here, there, mask)
        for d in range(4):
            for c in range(COMPS):
                src = component(refs, d, c)
                n = d * COMPS + c
                for out, k, r in ((down, 0, rows - 2), (down, 1, rows - 1), (up, 0, 0)):
                    per = 2 if out is down else 1
                    to = (n * per + k) * span
                    side = (n * rows + r) * 2
                    out[to : to + 2] = west[side : side + 2]
                    out[to + 2 : to + 2 + cols] = src[r]
                    out[to + 2 + cols : to + span] = east[side : side + 2]
        at = 4 * COMPS * 2 * span
        for k in range(12):
            up_t[2 * k : 2 * k + 2] = text[k * rows : k * rows + 2]
            down[at + 2 * k : at + 2 * k + 2] = text[(k + 1) * rows - 2 : (k + 1) * rows]

    n = 4 * COMPS
    return call(
        body,
        [(12 * rows, LANES), (24, LANES), (n * 2 * span + 24, LANES), (n * span, LANES)],
    )


def spread(row, out, k, at, span):
    full = -(-span // SUB) * SUB
    wide = jnp.broadcast_to(row, (full, LANES))
    picked = jnp.where(iota((full, LANES), 0) == iota((full, LANES), 1), wide, 0.0)
    value = jnp.broadcast_to(jnp.sum(picked, axis=1, keepdims=True), (full, LANES))
    out[k, at : at + span] = value[:span]


def apply_rows(affine, points):
    mapped = []
    for c in range(3):
        value = affine(4 * c + 3) + affine(4 * c) * points[0]
        value = value + affine(4 * c + 1) * points[1]
        mapped.append(value + affine(4 * c + 2) * points[2])
    return mapped


def squared(here, there):
    delta = [a - b for a, b in zip(here, there)]
    return delta[0] * delta[0] + delta[1] * delta[1] + delta[2] * delta[2]


def send_stats(out, largest, total, count):
    lane = iota(out.shape, len(out.shape) - 1)
    out[...] = jnp.where(lane == 0, largest, jnp.where(lane == 1, total, jnp.where(lane == 2, count, 0.0)))


def read_stats(got):
    values = got[...]
    lane = iota(values.shape, 2)
    largest = jnp.max(jnp.where(lane == 0, values, 0.0))
    total = jnp.sum(jnp.where(lane == 1, values, 0.0))
    count = jnp.sum(jnp.where(lane == 2, values, 0.0))
    return largest, total / jnp.maximum(count, 1.0)


def first_stats(rows, cols, devices):
    span = cols + 4

    def body(here, there, mask, text, up_t, out, rep):
        for k in range(12):
            for r in range(rows):
                spread(text[k * rows + r : k * rows + r + 1], rep, k, r * span, span)
            spread(up_t[2 * k : 2 * k + 1], rep, k, rows * span, span)
        top = jnp.zeros((cols, LANES), jnp.float32)
        total = jnp.zeros((cols, LANES), jnp.float32)
        count = jnp.zeros((cols, LANES), jnp.float32)
        for d, (dr, dc) in enumerate(link_offsets):
            for r in range(rows):
                near = r * span + 2
                far = (r + dr) * span + 2 + dc
                a = apply_rows(lambda k: rep[k, near : near + cols], [here[d, c, r] for c in range(3)])
                b = apply_rows(lambda k: rep[k, far : far + cols], [there[d, c, r] for c in range(3)])
                weight = mask[d, r]
                masked = weight * squared(a, b)
                top = jnp.maximum(top, masked)
                total = total + masked
                count = count + weight
        send_stats(out, jnp.max(top), jnp.sum(total), jnp.sum(count))

    pad = -(-((rows + 1) * span) // SUB) * SUB + SUB
    return call(body, [(devices, 1, LANES)], [(12, pad, LANES)])


class Flat:

    def __init__(self, rows, cols):
        self.rows, self.cols = rows, cols
        self.span = cols + 4
        self.tiles = -(-((rows + 4) * self.span + self.span + 1) // SUB) * SUB + 2 * SUB
        self.shift = [dr * self.span + dc for dr, dc in link_offsets]

    def at(self, r, c):
        return SUB + (r + 2) * self.span + c + 2

    def blocks(self, r0, c0, r1, c1):
        return range(self.at(r0, c0) // SUB * SUB, self.at(r1, c1) + 1, SUB)

    def owned(self, f):
        index = iota((SUB, LANES), 0) + f
        keep = None
        for r in range(self.rows):
            low, high = self.at(r, 0), self.at(r, self.cols - 1)
            if low <= f and f + SUB - 1 <= high:
                return True
            if low < f + SUB and high >= f:
                one = (index >= low) & (index <= high)
                keep = one if keep is None else keep | one
        return keep


def link_values(flat, f, d, points, rep, errors, here_out, there_out):
    near = slice(f, f + SUB)
    far = slice(f + flat.shift[d], f + flat.shift[d] + SUB)
    a = apply_rows(lambda k: rep[k, near], [points[d * COMPS + c, near] for c in range(3)])
    b = apply_rows(lambda k: rep[k, far], [points[d * COMPS + 3 + c, near] for c in range(3)])
    error = squared(a, b)
    errors[d, near] = error
    for c in range(3):
        here_out[3 * d + c, near] = a[c]
        there_out[3 * d + c, near] = b[c]
    return error


def assemble(rows, cols):
    flat = Flat(rows, cols)
    span = flat.span

    def body(here, there, mask, text, west, east, north, south, up_t, points, rep, errors, mapped, target):
        refs = (here, there, mask)
        for d in range(4):
            for c in range(COMPS):
                n = d * COMPS + c
                src = component(refs, d, c)
                at = flat.at(-2, -2)
                points[n, at : at + 2 * span] = north[n * 2 * span : (n + 1) * 2 * span]
                for r in range(rows):
                    at = flat.at(r, -2)
                    side = (n * rows + r) * 2
                    points[n, at : at + 2] = west[side : side + 2]
                    points[n, at + 2 : at + 2 + cols] = src[r]
                    points[n, at + 2 + cols : at + span] = east[side : side + 2]
                at = flat.at(rows, -2)
                points[n, at : at + span] = south[n * span : (n + 1) * span]
        north_t = 4 * COMPS * 2 * span
        for k in range(12):
            for j in range(2):
                row = north_t + 2 * k + j
                spread(north[row : row + 1], rep, k, flat.at(j - 2, -2), span)
                spread(up_t[2 * k + j : 2 * k + j + 1], rep, k, flat.at(rows + j, -2), span)
            for r in range(rows):
                spread(text[k * rows + r : k * rows + r + 1], rep, k, flat.at(r, -2), span)
        for f in flat.blocks(-2, -2, rows, cols + 1):
            for d in range(4):
                link_values(flat, f, d, points, rep, errors, mapped, target)

    t = flat.tiles
    return call(
        body,
        [(4 * COMPS, t, LANES), (12, t, LANES), (4, t, LANES), (12, t, LANES), (12, t, LANES)],
    )


def weigh(flat, blocks, points, errors, weights, scale):
    for f in blocks:
        for d in range(4):
            weights[d, f : f + SUB] = points[d * COMPS + 6, f : f + SUB] * scale / (scale + errors[d, f : f + SUB])


def tile_sums(flat, f, points, mapped, target, weights):
    gram = {}
    cross = {}

    def put(store, key, value):
        store[key] = value if key not in store else store[key] + value

    for d in range(4):
        for end in range(2):
            at = f if end == 0 else f - flat.shift[d]
            rows = slice(at, at + SUB)
            base = d * COMPS + 3 * end
            x = [points[base + c, rows] for c in range(3)]
            other = target if end == 0 else mapped
            weight = weights[d, rows]
            weighted = [weight * v for v in x] + [weight]
            for a, b in GRAM:
                if a == 3:
                    put(gram, (a, b), weighted[b])
                else:
                    put(gram, (a, b), weighted[a] * x[b])
            for c in range(3):
                scaled = weight * other[3 * d + c, rows]
                put(cross, (c, 3), scaled)
                for b in range(3):
                    put(cross, (c, b), scaled * x[b])

    def lanes(v):
        return jnp.broadcast_to(jnp.sum(v, axis=1, keepdims=True), v.shape)

    return {k: lanes(v) for k, v in gram.items()}, {k: lanes(v) for k, v in cross.items()}


def solve_small(gram, cross):
    factor = {}
    inverse = {}
    for a in range(4):
        for b in range(a + 1):
            value = gram[a, b]
            for i in range(b):
                value = value - factor[a, i] * factor[b, i]
            if a == b:
                inverse[a] = 1.0 / jnp.sqrt(value)
            else:
                factor[a, b] = value * inverse[b]
    result = []
    for c in range(3):
        forward = []
        for a in range(4):
            value = cross[c, a]
            for i in range(a):
                value = value - factor[a, i] * forward[i]
            forward.append(value * inverse[a])
        backward = [None] * 4
        for a in (3, 2, 1, 0):
            value = forward[a]
            for i in range(a + 1, 4):
                value = value - factor[i, a] * backward[i]
            backward[a] = value * inverse[a]
        result.extend(backward)
    return result


def update(flat, blocks, points, rep, mapped, target, weights, damping, out):
    for f in blocks:
        gram, cross = tile_sums(flat, f, points, mapped, target, weights)
        for a in range(4):
            gram[a, a] = gram[a, a] + damping
        for c in range(3):
            for b in range(4):
                cross[c, b] = cross[c, b] + damping * rep[4 * c + b, f : f + SUB]
        for k, value in enumerate(solve_small(gram, cross)):
            out[k, f : f + SUB] = value


def first_update(rows, cols, devices):
    flat = Flat(rows, cols)

    def body(got, points, rep, errors, mapped, target, new_rep, new_errors, new_mapped, new_target, out, weights):
        largest, mean_error = read_stats(got)
        scale = 0.25 * largest + 1e-06
        damping = damping_scale * mean_error + 1.0
        weigh(flat, flat.blocks(-2, -2, rows, cols + 1), points, errors, weights, scale)
        update(flat, flat.blocks(-1, -1, rows, cols), points, rep, mapped, target, weights, damping, new_rep)
        zero = jnp.zeros((SUB, LANES), jnp.float32)
        top, total, count = zero, zero, zero
        for f in flat.blocks(-1, -1, rows - 1, cols):
            keep = flat.owned(f)
            for d in range(4):
                error = link_values(flat, f, d, points, new_rep, new_errors, new_mapped, new_target)
                if keep is None:
                    continue
                weight = points[d * COMPS + 6, f : f + SUB]
                masked = weight * error
                if keep is not True:
                    masked = jnp.where(keep, masked, 0.0)
                    weight = jnp.where(keep, weight, 0.0)
                top = jnp.maximum(top, masked)
                total = total + masked
                count = count + weight
        send_stats(out, jnp.max(top), jnp.sum(total), jnp.sum(count))

    t = flat.tiles
    return call(
        body,
        [(12, t, LANES), (4, t, LANES), (12, t, LANES), (12, t, LANES), (devices, 1, LANES)],
        [(4, t, LANES)],
    )


def last_update(rows, cols):
    flat = Flat(rows, cols)

    def body(got0, got1, points, rep, errors, mapped, target, aligned, stats, weights, new_rep):
        first, mean0 = read_stats(got0)
        largest, mean_error = read_stats(got1)
        scale = 0.25 * largest + 1e-06
        damping = damping_scale * mean_error + 1.0
        weigh(flat, flat.blocks(-1, -1, rows - 1, cols), points, errors, weights, scale)
        update(flat, flat.blocks(0, 0, rows - 1, cols - 1), points, rep, mapped, target, weights, damping, new_rep)
        diagonal = iota((cols, LANES), 0) == iota((cols, LANES), 1)
        for k in range(12):
            for r in range(rows):
                at = flat.at(r, 0)
                value = jnp.where(diagonal, new_rep[k, at : at + cols], 0.0)
                aligned[k, r : r + 1] = jnp.sum(value, axis=0, keepdims=True)[:, 0:cols]
        row = iota((2, 2), 0)
        col = iota((2, 2), 1)
        stats[...] = jnp.where(row == 0, jnp.where(col == 0, first, largest), jnp.where(col == 0, mean0, mean_error))

    t = flat.tiles
    return call(body, [(12, rows, cols), (2, 2)], [(4, t, LANES), (12, t, LANES)])


def onward(array, axis, by):
    peers = lax.axis_size(axis)
    return lax.ppermute(array, axis, [(i, i + by) for i in range(peers) if 0 <= i + by < peers])


def everyone(array):
    return lax.all_to_all(array, ("row", "col"), 0, 0)


def on_device(points_here, points_there, outlier_mask, transforms):
    rows, cols = transforms.shape[2:]
    devices = lax.axis_size("row") * lax.axis_size("col")
    flat_transforms = transforms.reshape(12 * rows, cols)
    mask, to_east, to_west = pack_cols(rows, cols)(points_here, points_there, outlier_mask, flat_transforms)
    west = onward(to_east, "col", 1)
    east = onward(to_west, "col", -1)
    text, to_up_t, to_down, to_up = pack_rows(rows, cols)(
        points_here, points_there, mask, flat_transforms, west, east
    )
    up_t = onward(to_up_t, "row", -1)
    north = onward(to_down, "row", 1)
    south = onward(to_up, "row", -1)
    (sent,) = first_stats(rows, cols, devices)(points_here, points_there, mask, text, up_t)
    got0 = everyone(sent)
    points, rep, errors, mapped, target = assemble(rows, cols)(
        points_here, points_there, mask, text, west, east, north, south, up_t
    )
    rep, errors, mapped, target, sent = first_update(rows, cols, devices)(
        got0, points, rep, errors, mapped, target
    )
    got1 = everyone(sent)
    aligned, stats = last_update(rows, cols)(got0, got1, points, rep, errors, mapped, target)
    return aligned.reshape(3, 4, rows, cols), stats


def solution(mesh):
    return jax.shard_map(
        on_device,
        mesh=mesh,
        in_specs=(
            P(None, None, "row", "col", None),
            P(None, None, "row", "col", None),
            P(None, "row", "col", None),
            P(None, None, "row", "col"),
        ),
        out_specs=(P(None, None, "row", "col"), P()),
        check_vma=False,
    )
```

```python
import jax
import jax.numpy as jnp
from jax import lax
from jax.experimental import pallas as pl
from jax.experimental.pallas import tpu as pltpu
from jax.sharding import PartitionSpec as P

LANES = 128
SUB = 8
COMPS = 7

link_offsets = ((0, 1), (1, 0), (1, 1), (1, -1))
damping_scale = 64.0
GRAM = [(a, b) for a in range(4) for b in range(a + 1)]


def call(body, out_shapes, scratch=(), in_vmem=(), in_hbm=(), aliases=None, results=pltpu.VMEM):
    shapes = [(results or jax.ShapeDtypeStruct)(s, jnp.float32) for s in out_shapes]
    vmem = pl.BlockSpec(memory_space=pltpu.VMEM)
    hbm = pl.BlockSpec(memory_space=pltpu.HBM)

    def run(*args):
        spaces = {**dict.fromkeys(in_vmem, pltpu.VMEM), **dict.fromkeys(in_hbm, pltpu.HBM)}
        args = [pltpu.with_memory_space_constraint(v, spaces[i]) if i in spaces else v for i, v in enumerate(args)]
        return pl.pallas_call(
            body,
            out_shape=shapes,
            in_specs=[hbm if i in in_hbm else vmem for i in range(len(args))],
            out_specs=[vmem] * len(shapes),
            scratch_shapes=[pltpu.VMEM(s, jnp.float32) if isinstance(s, tuple) else s for s in scratch],
            input_output_aliases=aliases or {},
            compiler_params=pltpu.CompilerParams(vmem_limit_bytes=16 * 1024 * 1024),
        )(*args)

    return run


def iota(shape, axis):
    return lax.broadcasted_iota(jnp.int32, shape, axis)


WEST_LINKS = [(0, d) for d in (0, 2)] + [(1, d) for d in range(4)]
EAST_LINKS = [(0, d) for d in range(4)] + [(1, 3)]


def side_rows(links, rows):
    return [(d, j, c, (n * COMPS + c) * rows) for n, (j, d) in enumerate(links) for c in range(COMPS)]


def pack_cols(flat):
    rows, cols = flat.rows, flat.cols
    groups = 12 * rows // SUB

    def body(here_in, there_in, outlier_in, transforms_in, points, padded, to_east, to_west, *scratch):
        here, there, outlier, transforms, sems = scratch
        copies = []
        for n, (source, goal) in enumerate(((here_in, here), (there_in, there), (outlier_in, outlier))):
            copies.append([pltpu.make_async_copy(source.at[d], goal.at[d], sems.at[n, d]) for d in range(4)])
        copies.append([pltpu.make_async_copy(transforms_in, transforms, sems.at[3, 0])])
        for d in range(4):
            for n in range(3):
                copies[n][d].start()
        copies[3][0].start()
        grid_rows = rows * lax.axis_size("row")
        grid_cols = cols * lax.axis_size("col")
        row0 = lax.axis_index("row") * rows
        col_ids = lax.axis_index("col") * cols + iota((cols, LANES), 0)
        for d, (dr, dc) in enumerate(link_offsets):
            col_valid = jnp.where((col_ids + dc >= 0) & (col_ids + dc < grid_cols), 1.0, 0.0)
            for n in range(3):
                copies[n][d].wait()
            for r in range(rows):
                own = slice(flat.at(r, 0), flat.at(r, cols))
                row_valid = jnp.where(row0 + r + dr < grid_rows, 1.0, 0.0)
                points[d * COMPS + 6, own] = outlier[d, r].astype(jnp.float32) * (col_valid * row_valid)
                for c in range(3):
                    points[d * COMPS + c, own] = here[d, c, r]
                    points[d * COMPS + 3 + c, own] = there[d, c, r]
        for out, links, first in ((to_east, WEST_LINKS, cols - 2), (to_west, EAST_LINKS, 0)):
            for d, j, c, at in side_rows(links, rows):
                for r in range(rows):
                    tile = flat.at(r, first + j)
                    out[at + r : at + r + 1] = points[d * COMPS + c, tile : tile + 1]
        padded[...] = jnp.zeros((12 * rows, LANES), jnp.float32)
        copies[3][0].wait()
        padded[:, 0:cols] = transforms[...]
        lane = iota((SUB, LANES), 1)
        for out, links, first in ((to_east, WEST_LINKS, cols - 2), (to_west, EAST_LINKS, 0)):
            packed = jnp.zeros((SUB, LANES), jnp.float32)
            for g in range(groups):
                moved = pltpu.roll(padded[g * SUB : (g + 1) * SUB], (2 * g - first) % LANES, 1)
                packed = jnp.where((lane == 2 * g) | (lane == 2 * g + 1), moved, packed)
            out[len(links) * COMPS * rows :] = packed

    count = [len(links) * COMPS * rows + SUB for links in (WEST_LINKS, EAST_LINKS)]
    return call(
        body,
        [(4 * COMPS, flat.tiles, LANES), (12 * rows, LANES), (count[0], LANES), (count[1], LANES)],
        [
            pltpu.VMEM((4, 3, rows, cols, LANES), jnp.float32),
            pltpu.VMEM((4, 3, rows, cols, LANES), jnp.float32),
            pltpu.VMEM((4, rows, cols, LANES), jnp.int32),
            pltpu.VMEM((12 * rows, cols), jnp.float32),
            pltpu.SemaphoreType.DMA((4, 4)),
        ],
        in_hbm=range(4),
    )


def pack_corner_rows(flat):
    rows, cols = flat.rows, flat.cols

    def body(padded, west, east, text, up_t):
        lane = iota((SUB, LANES), 1)
        from_west = west[len(WEST_LINKS) * COMPS * rows :]
        from_east = east[len(EAST_LINKS) * COMPS * rows :]
        for g in range(12 * rows // SUB):
            part = slice(g * SUB, (g + 1) * SUB)
            left = pltpu.roll(from_west, -2 * g % LANES, 1)
            right = pltpu.roll(from_east, (cols + 2 - 2 * g) % LANES, 1)
            own = pltpu.roll(padded[part], 2, 1)
            value = jnp.where(lane < 2, left, jnp.where(lane < cols + 2, own, right))
            text[part] = jnp.where(lane < flat.span, value, 0.0)
        for k in range(12):
            up_t[2 * k : 2 * k + 2] = text[k * rows : k * rows + 2]

    return call(body, [(12 * rows, LANES), (24, LANES)], in_vmem=(0, 1, 2))


def north_slices(flat):
    span, at, found = flat.span, 0, []
    for d in range(4):
        for c in range(COMPS):
            count = 1 if d == 0 else 2
            found.append((d * COMPS + c, 2 - count, count * span, at))
            at += count * span
    return found, at


def pack_rows(flat):
    rows, cols, span = flat.rows, flat.cols, flat.span
    slices, north_t = north_slices(flat)

    def body(points_in, west, east, text, points, down, up):
        for side, links, first in ((west, WEST_LINKS, -2), (east, EAST_LINKS, cols)):
            for d, j, c, at in side_rows(links, rows):
                for r in range(rows):
                    tile = flat.at(r, first + j)
                    points[d * COMPS + c, tile : tile + 1] = side[at + r : at + r + 1]
        for n, skip, count, to in slices:
            at = flat.at(rows - 2 + skip, -2)
            down[to : to + count] = points[n, at : at + count]
        for n in range(4 * COMPS):
            up[n * span : (n + 1) * span] = points[n, flat.at(0, -2) : flat.at(0, -2) + span]
        for k in range(12):
            down[north_t + 2 * k : north_t + 2 * k + 2] = text[(k + 1) * rows - 2 : (k + 1) * rows]

    return call(
        body,
        [(4 * COMPS, flat.tiles, LANES), (north_t + 24, LANES), (4 * COMPS * span, LANES)],
        in_vmem=(0, 1, 2, 3),
        aliases={0: 0},
    )


def spread(row, out, k, at, span):
    full = -(-span // SUB) * SUB
    wide = jnp.broadcast_to(row, (full, LANES))
    picked = jnp.where(iota((full, LANES), 0) == iota((full, LANES), 1), wide, 0.0)
    value = jnp.broadcast_to(jnp.sum(picked, axis=1, keepdims=True), (full, LANES))
    out[k, at : at + span] = value[:span]


def apply_rows(affine, points):
    mapped = []
    for c in range(3):
        value = affine(4 * c + 3) + affine(4 * c) * points[0]
        value = value + affine(4 * c + 1) * points[1]
        mapped.append(value + affine(4 * c + 2) * points[2])
    return mapped


def squared(here, there):
    delta = [a - b for a, b in zip(here, there)]
    return delta[0] * delta[0] + delta[1] * delta[1] + delta[2] * delta[2]


def send_stats(out, largest, total, count):
    lane = iota(out.shape, len(out.shape) - 1)
    out[...] = jnp.where(lane == 0, largest, jnp.where(lane == 1, total, jnp.where(lane == 2, count, 0.0)))


def read_stats(got):
    values = got[...]
    lane = iota(values.shape, 2)
    largest = jnp.max(jnp.where(lane == 0, values, 0.0))
    total = jnp.sum(jnp.where(lane == 1, values, 0.0))
    count = jnp.sum(jnp.where(lane == 2, values, 0.0))
    return largest, total / jnp.maximum(count, 1.0)


class Flat:

    def __init__(self, rows, cols):
        self.rows, self.cols = rows, cols
        self.span = cols + 4
        self.tiles = -(-((rows + 4) * self.span + self.span + 1) // SUB) * SUB + 2 * SUB
        self.shift = [dr * self.span + dc for dr, dc in link_offsets]

    def at(self, r, c):
        return SUB + (r + 2) * self.span + c + 2

    def blocks(self, r0, c0, r1, c1):
        return range(self.at(r0, c0) // SUB * SUB, self.at(r1, c1) + 1, SUB)

    def own_blocks(self):
        return self.blocks(0, 0, self.rows - 1, self.cols - 1)

    def owned(self, f):
        index = iota((SUB, LANES), 0) + f
        keep = None
        for r in range(self.rows):
            low, high = self.at(r, 0), self.at(r, self.cols - 1)
            if low <= f and f + SUB - 1 <= high:
                return True
            if low < f + SUB and high >= f:
                one = (index >= low) & (index <= high)
                keep = one if keep is None else keep | one
        return keep


def link_values(flat, f, d, points, rep, errors, here_out, there_out):
    near = slice(f, f + SUB)
    far = slice(f + flat.shift[d], f + flat.shift[d] + SUB)
    a = apply_rows(lambda k: rep[k, near], [points[d * COMPS + c, near] for c in range(3)])
    b = apply_rows(lambda k: rep[k, far], [points[d * COMPS + 3 + c, near] for c in range(3)])
    error = squared(a, b)
    errors[d, near] = error
    for c in range(3):
        here_out[3 * d + c, near] = a[c]
        there_out[3 * d + c, near] = b[c]
    return error


def own_stats(flat, points, rep, errors, mapped, target, blocks, out):
    zero = jnp.zeros((SUB, LANES), jnp.float32)
    top, total, count = zero, zero, zero
    for f in blocks:
        keep = flat.owned(f)
        for d in range(4):
            error = link_values(flat, f, d, points, rep, errors, mapped, target)
            if keep is None:
                continue
            weight = points[d * COMPS + 6, f : f + SUB]
            masked = weight * error
            if keep is not True:
                masked = jnp.where(keep, masked, 0.0)
                weight = jnp.where(keep, weight, 0.0)
            top = jnp.maximum(top, masked)
            total = total + masked
            count = count + weight
    send_stats(out, jnp.max(top), jnp.sum(total), jnp.sum(count))


def first_stats(flat, devices):
    rows = flat.rows

    def body(points, text, up_t, rep, errors, mapped, target, out):
        for k in range(12):
            for r in range(rows):
                spread(text[k * rows + r : k * rows + r + 1], rep, k, flat.at(r, -2), flat.span)
            spread(up_t[2 * k : 2 * k + 1], rep, k, flat.at(rows, -2), flat.span)
        own_stats(flat, points, rep, errors, mapped, target, flat.own_blocks(), out)

    t = flat.tiles
    return call(
        body,
        [(12, t, LANES), (4, t, LANES), (12, t, LANES), (12, t, LANES), (devices, 1, LANES)],
        in_vmem=(0, 1, 2),
    )


def outer_values(flat, points, rep, errors, mapped, target, north, south, up_t):
    rows, span = flat.rows, flat.span
    slices, north_t = north_slices(flat)
    for n, skip, count, src in slices:
        at = flat.at(skip - 2, -2)
        points[n, at : at + count] = north[src : src + count]
    for n in range(4 * COMPS):
        at = flat.at(rows, -2)
        points[n, at : at + span] = south[n * span : (n + 1) * span]
    for k in range(12):
        for j in range(2):
            row = north_t + 2 * k + j
            spread(north[row : row + 1], rep, k, flat.at(j - 2, -2), span)
        spread(up_t[2 * k + 1 : 2 * k + 2], rep, k, flat.at(rows + 1, -2), span)
    inner = set(flat.own_blocks())
    for f in flat.blocks(-2, -2, rows, flat.cols + 1):
        if f not in inner:
            for d in range(4):
                link_values(flat, f, d, points, rep, errors, mapped, target)


def weigh(blocks, points, errors, weights, scale):
    for f in blocks:
        for d in range(4):
            weights[d, f : f + SUB] = points[d * COMPS + 6, f : f + SUB] * scale / (scale + errors[d, f : f + SUB])


def tile_sums(flat, f, points, mapped, target, weights):
    gram = {}
    cross = {}

    def put(store, key, value):
        store[key] = value if key not in store else store[key] + value

    for d in range(4):
        for end in range(2):
            at = f if end == 0 else f - flat.shift[d]
            rows = slice(at, at + SUB)
            base = d * COMPS + 3 * end
            x = [points[base + c, rows] for c in range(3)]
            other = target if end == 0 else mapped
            weight = weights[d, rows]
            weighted = [weight * v for v in x] + [weight]
            for a, b in GRAM:
                if a == 3:
                    put(gram, (a, b), weighted[b])
                else:
                    put(gram, (a, b), weighted[a] * x[b])
            for c in range(3):
                scaled = weight * other[3 * d + c, rows]
                put(cross, (c, 3), scaled)
                for b in range(3):
                    put(cross, (c, b), scaled * x[b])

    def lanes(v):
        return jnp.broadcast_to(jnp.sum(v, axis=1, keepdims=True), v.shape)

    return {k: lanes(v) for k, v in gram.items()}, {k: lanes(v) for k, v in cross.items()}


def solve_small(gram, cross):
    factor = {}
    inverse = {}
    for a in range(4):
        for b in range(a + 1):
            value = gram[a, b]
            for i in range(b):
                value = value - factor[a, i] * factor[b, i]
            if a == b:
                inverse[a] = 1.0 / jnp.sqrt(value)
            else:
                factor[a, b] = value * inverse[b]
    result = []
    for c in range(3):
        forward = []
        for a in range(4):
            value = cross[c, a]
            for i in range(a):
                value = value - factor[a, i] * forward[i]
            forward.append(value * inverse[a])
        backward = [None] * 4
        for a in (3, 2, 1, 0):
            value = forward[a]
            for i in range(a + 1, 4):
                value = value - factor[i, a] * backward[i]
            backward[a] = value * inverse[a]
        result.extend(backward)
    return result


def update(flat, blocks, points, rep, mapped, target, weights, damping, out):
    for f in blocks:
        gram, cross = tile_sums(flat, f, points, mapped, target, weights)
        for a in range(4):
            gram[a, a] = gram[a, a] + damping
        for c in range(3):
            for b in range(4):
                cross[c, b] = cross[c, b] + damping * rep[4 * c + b, f : f + SUB]
        for k, value in enumerate(solve_small(gram, cross)):
            out[k, f : f + SUB] = value


def first_update(flat, devices):
    rows, cols = flat.rows, flat.cols

    def body(*refs):
        got, north, south, up_t = refs[5:9]
        points, rep, errors, mapped, target, new_rep, out, weights = refs[9:]
        state = (points, rep, errors, mapped, target)
        outer_values(flat, *state, north, south, up_t)
        largest, mean_error = read_stats(got)
        scale = 0.25 * largest + 1e-06
        damping = damping_scale * mean_error + 1.0
        weigh(flat.blocks(-2, -2, rows, cols + 1), points, errors, weights, scale)
        update(flat, flat.blocks(-1, -1, rows, cols), points, rep, mapped, target, weights, damping, new_rep)
        blocks = flat.blocks(-1, -1, rows - 1, cols)
        own_stats(flat, points, new_rep, errors, mapped, target, blocks, out)

    t = flat.tiles
    return call(
        body,
        [(4 * COMPS, t, LANES)] + [(n, t, LANES) for n in (12, 4, 12, 12, 12)] + [(devices, 1, LANES)],
        [(4, t, LANES)],
        in_vmem=range(9),
        aliases={i: i for i in range(5)},
    )


def last_update(flat):
    rows, cols = flat.rows, flat.cols

    def body(got0, got1, points, rep, errors, mapped, target, aligned, stats, weights, new_rep):
        first, mean0 = read_stats(got0)
        largest, mean_error = read_stats(got1)
        scale = 0.25 * largest + 1e-06
        damping = damping_scale * mean_error + 1.0
        weigh(flat.blocks(-1, -1, rows - 1, cols), points, errors, weights, scale)
        update(flat, flat.blocks(0, 0, rows - 1, cols - 1), points, rep, mapped, target, weights, damping, new_rep)
        diagonal = iota((cols, LANES), 0) == iota((cols, LANES), 1)
        for k in range(12):
            for r in range(rows):
                at = flat.at(r, 0)
                value = jnp.where(diagonal, new_rep[k, at : at + cols], 0.0)
                aligned[k, r : r + 1] = jnp.sum(value, axis=0, keepdims=True)[:, 0:cols]
        row = iota((2, 2), 0)
        col = iota((2, 2), 1)
        stats[...] = jnp.where(row == 0, jnp.where(col == 0, first, largest), jnp.where(col == 0, mean0, mean_error))

    t = flat.tiles
    return call(body, [(12, rows, cols), (2, 2)], [(4, t, LANES), (12, t, LANES)], in_vmem=range(7), results=None)


def onward(array, axis, by):
    peers = lax.axis_size(axis)
    return lax.ppermute(array, axis, [(i, i + by) for i in range(peers) if 0 <= i + by < peers])


def everyone(array):
    return lax.all_to_all(array, ("row", "col"), 0, 0)


def on_device(points_here, points_there, outlier_mask, transforms):
    rows, cols = transforms.shape[2:]
    devices = lax.axis_size("row") * lax.axis_size("col")
    flat = Flat(rows, cols)
    points, padded, to_east, to_west = pack_cols(flat)(
        points_here, points_there, outlier_mask, transforms.reshape(12 * rows, cols)
    )
    west = onward(to_east, "col", 1)
    east = onward(to_west, "col", -1)
    text, to_up_t = pack_corner_rows(flat)(padded, west, east)
    up_t = onward(to_up_t, "row", -1)
    points, to_down, to_up = pack_rows(flat)(points, west, east, text)
    north = onward(to_down, "row", 1)
    south = onward(to_up, "row", -1)
    rep, errors, mapped, target, sent = first_stats(flat, devices)(points, text, up_t)
    got0 = everyone(sent)
    points, _, errors, mapped, target, rep, sent = first_update(flat, devices)(
        points, rep, errors, mapped, target, got0, north, south, up_t
    )
    got1 = everyone(sent)
    aligned, stats = last_update(flat)(got0, got1, points, rep, errors, mapped, target)
    return aligned.reshape(3, 4, rows, cols), stats


def solution(mesh):
    return jax.shard_map(
        on_device,
        mesh=mesh,
        in_specs=(
            P(None, None, "row", "col", None),
            P(None, None, "row", "col", None),
            P(None, "row", "col", None),
            P(None, None, "row", "col"),
        ),
        out_specs=(P(None, None, "row", "col"), P()),
        check_vma=False,
    )
```

```python
import jax
import jax.numpy as jnp
from jax import lax
from jax.experimental import pallas as pl
from jax.experimental.pallas import tpu as pltpu
from jax.sharding import PartitionSpec as P

LANES = 128
SUB = 8
COMPS = 7

link_offsets = ((0, 1), (1, 0), (1, 1), (1, -1))
damping_scale = 64.0
GRAM = [(a, b) for a in range(4) for b in range(a + 1)]


def call(body, out_shapes, scratch=(), in_vmem=(), in_hbm=(), aliases=None, results=pltpu.VMEM):
    shapes = [(results or jax.ShapeDtypeStruct)(s, jnp.float32) for s in out_shapes]
    vmem = pl.BlockSpec(memory_space=pltpu.VMEM)
    hbm = pl.BlockSpec(memory_space=pltpu.HBM)

    def run(*args):
        spaces = {**dict.fromkeys(in_vmem, pltpu.VMEM), **dict.fromkeys(in_hbm, pltpu.HBM)}
        args = [pltpu.with_memory_space_constraint(v, spaces[i]) if i in spaces else v for i, v in enumerate(args)]
        return pl.pallas_call(
            body,
            out_shape=shapes,
            in_specs=[hbm if i in in_hbm else vmem for i in range(len(args))],
            out_specs=[vmem] * len(shapes),
            scratch_shapes=[pltpu.VMEM(s, jnp.float32) if isinstance(s, tuple) else s for s in scratch],
            input_output_aliases=aliases or {},
            compiler_params=pltpu.CompilerParams(vmem_limit_bytes=16 * 1024 * 1024),
        )(*args)

    return run


def iota(shape, axis):
    return lax.broadcasted_iota(jnp.int32, shape, axis)


WEST_LINKS = [(0, d) for d in (0, 2)] + [(1, d) for d in range(4)]
EAST_LINKS = [(0, d) for d in range(4)] + [(1, 3)]


def side_rows(links, rows):
    return [(d, j, c, (n * COMPS + c) * rows) for n, (j, d) in enumerate(links) for c in range(COMPS)]


def side_count(rows):
    return max(len(WEST_LINKS), len(EAST_LINKS)) * COMPS * rows + SUB


def by_parity(axis, body, first, second):
    odd = lax.rem(lax.axis_index(axis), 2)

    @pl.when(odd == 0)
    def _():
        body(first, second)

    @pl.when(odd == 1)
    def _():
        body(second, first)


def swap(array, axis, first):
    peers = lax.axis_size(axis)
    lower = range(first, peers - 1, 2)
    return lax.ppermute(array, axis, [pair for i in lower for pair in ((i, i + 1), (i + 1, i))])


def pack_cols(flat):
    rows, cols = flat.rows, flat.cols
    groups = 12 * rows // SUB

    def body(here_in, there_in, outlier_in, transforms_in, points, padded, first_swap, second_swap, *scratch):
        here, there, outlier, transforms, sems = scratch
        copies = []
        for n, (source, goal) in enumerate(((here_in, here), (there_in, there), (outlier_in, outlier))):
            copies.append([pltpu.make_async_copy(source.at[d], goal.at[d], sems.at[n, d]) for d in range(4)])
        copies.append([pltpu.make_async_copy(transforms_in, transforms, sems.at[3, 0])])
        for d in range(4):
            for n in range(3):
                copies[n][d].start()
        copies[3][0].start()
        grid_rows = rows * lax.axis_size("row")
        grid_cols = cols * lax.axis_size("col")
        row0 = lax.axis_index("row") * rows
        col_ids = lax.axis_index("col") * cols + iota((cols, LANES), 0)
        for d, (dr, dc) in enumerate(link_offsets):
            col_valid = jnp.where((col_ids + dc >= 0) & (col_ids + dc < grid_cols), 1.0, 0.0)
            for n in range(3):
                copies[n][d].wait()
            for r in range(rows):
                own = slice(flat.at(r, 0), flat.at(r, cols))
                row_valid = jnp.where(row0 + r + dr < grid_rows, 1.0, 0.0)
                points[d * COMPS + 6, own] = outlier[d, r].astype(jnp.float32) * (col_valid * row_valid)
                for c in range(3):
                    points[d * COMPS + c, own] = here[d, c, r]
                    points[d * COMPS + 3 + c, own] = there[d, c, r]

        def pack_points(to_east, to_west):
            for out, links, first in ((to_east, WEST_LINKS, cols - 2), (to_west, EAST_LINKS, 0)):
                for d, j, c, at in side_rows(links, rows):
                    for r in range(rows):
                        tile = flat.at(r, first + j)
                        out[at + r : at + r + 1] = points[d * COMPS + c, tile : tile + 1]

        by_parity("col", pack_points, first_swap, second_swap)
        padded[...] = jnp.zeros((12 * rows, LANES), jnp.float32)
        copies[3][0].wait()
        padded[:, 0:cols] = transforms[...]
        lane = iota((SUB, LANES), 1)
        packed = []
        for first in (cols - 2, 0):
            value = jnp.zeros((SUB, LANES), jnp.float32)
            for g in range(groups):
                moved = pltpu.roll(padded[g * SUB : (g + 1) * SUB], (2 * g - first) % LANES, 1)
                value = jnp.where((lane == 2 * g) | (lane == 2 * g + 1), moved, value)
            packed.append(value)

        def pack_transforms(to_east, to_west):
            to_east[side_count(rows) - SUB :] = packed[0]
            to_west[side_count(rows) - SUB :] = packed[1]

        by_parity("col", pack_transforms, first_swap, second_swap)

    count = side_count(rows)
    return call(
        body,
        [(4 * COMPS, flat.tiles, LANES), (12 * rows, LANES), (count, LANES), (count, LANES)],
        [
            pltpu.VMEM((4, 3, rows, cols, LANES), jnp.float32),
            pltpu.VMEM((4, 3, rows, cols, LANES), jnp.float32),
            pltpu.VMEM((4, rows, cols, LANES), jnp.int32),
            pltpu.VMEM((12 * rows, cols), jnp.float32),
            pltpu.SemaphoreType.DMA((4, 4)),
        ],
        in_hbm=range(4),
    )


def north_slices(flat):
    span, at, found = flat.span, 0, []
    for d in range(4):
        for c in range(COMPS):
            count = 1 if d == 0 else 2
            found.append((d * COMPS + c, 2 - count, count * span, at))
            at += count * span
    return found, at


def pack_rows(flat):
    rows, cols, span = flat.rows, flat.cols, flat.span
    slices, north_t = north_slices(flat)
    south_t = 4 * COMPS * span

    def body(points_in, padded, first_swap, second_swap, points, text, down, up):
        def unpack(east, west):
            for side, links, first in ((west, WEST_LINKS, -2), (east, EAST_LINKS, cols)):
                for d, j, c, at in side_rows(links, rows):
                    for r in range(rows):
                        tile = flat.at(r, first + j)
                        points[d * COMPS + c, tile : tile + 1] = side[at + r : at + r + 1]
            lane = iota((SUB, LANES), 1)
            from_west = west[side_count(rows) - SUB :]
            from_east = east[side_count(rows) - SUB :]
            for g in range(12 * rows // SUB):
                part = slice(g * SUB, (g + 1) * SUB)
                left = pltpu.roll(from_west, -2 * g % LANES, 1)
                right = pltpu.roll(from_east, (cols + 2 - 2 * g) % LANES, 1)
                own = pltpu.roll(padded[part], 2, 1)
                value = jnp.where(lane < 2, left, jnp.where(lane < cols + 2, own, right))
                text[part] = jnp.where(lane < span, value, 0.0)

        by_parity("col", unpack, first_swap, second_swap)
        for n in range(4 * COMPS):
            up[n * span : (n + 1) * span] = points[n, flat.at(0, -2) : flat.at(0, -2) + span]
        for k in range(12):
            up[south_t + 2 * k : south_t + 2 * k + 2] = text[k * rows : k * rows + 2]
        for n, skip, count, to in slices:
            at = flat.at(rows - 2 + skip, -2)
            down[to : to + count] = points[n, at : at + count]
        for k in range(12):
            down[north_t + 2 * k : north_t + 2 * k + 2] = text[(k + 1) * rows - 2 : (k + 1) * rows]

    return call(
        body,
        [(4 * COMPS, flat.tiles, LANES), (12 * rows, LANES), (north_t + 24, LANES), (south_t + 24, LANES)],
        in_vmem=(0, 1, 2, 3),
        aliases={0: 0},
    )


def spread(row, out, k, at, span):
    full = -(-span // SUB) * SUB
    wide = jnp.broadcast_to(row, (full, LANES))
    picked = jnp.where(iota((full, LANES), 0) == iota((full, LANES), 1), wide, 0.0)
    value = jnp.broadcast_to(jnp.sum(picked, axis=1, keepdims=True), (full, LANES))
    out[k, at : at + span] = value[:span]


def apply_rows(affine, points):
    mapped = []
    for c in range(3):
        value = affine(4 * c + 3) + affine(4 * c) * points[0]
        value = value + affine(4 * c + 1) * points[1]
        mapped.append(value + affine(4 * c + 2) * points[2])
    return mapped


def squared(here, there):
    delta = [a - b for a, b in zip(here, there)]
    return delta[0] * delta[0] + delta[1] * delta[1] + delta[2] * delta[2]


def send_stats(out, largest, total, count):
    lane = iota(out.shape, len(out.shape) - 1)
    out[...] = jnp.where(lane == 0, largest, jnp.where(lane == 1, total, jnp.where(lane == 2, count, 0.0)))


def read_stats(got):
    values = got[...]
    lane = iota(values.shape, 2)
    largest = jnp.max(jnp.where(lane == 0, values, 0.0))
    total = jnp.sum(jnp.where(lane == 1, values, 0.0))
    count = jnp.sum(jnp.where(lane == 2, values, 0.0))
    return largest, total / jnp.maximum(count, 1.0)


class Flat:

    def __init__(self, rows, cols):
        self.rows, self.cols = rows, cols
        self.span = cols + 4
        self.tiles = -(-((rows + 4) * self.span + self.span + 1) // SUB) * SUB + 2 * SUB
        self.shift = [dr * self.span + dc for dr, dc in link_offsets]

    def at(self, r, c):
        return SUB + (r + 2) * self.span + c + 2

    def blocks(self, r0, c0, r1, c1):
        return range(self.at(r0, c0) // SUB * SUB, self.at(r1, c1) + 1, SUB)

    def own_blocks(self):
        return self.blocks(0, 0, self.rows - 1, self.cols - 1)

    def owned(self, f):
        index = iota((SUB, LANES), 0) + f
        keep = None
        for r in range(self.rows):
            low, high = self.at(r, 0), self.at(r, self.cols - 1)
            if low <= f and f + SUB - 1 <= high:
                return True
            if low < f + SUB and high >= f:
                one = (index >= low) & (index <= high)
                keep = one if keep is None else keep | one
        return keep


def link_values(flat, f, d, points, rep, errors, here_out, there_out):
    near = slice(f, f + SUB)
    far = slice(f + flat.shift[d], f + flat.shift[d] + SUB)
    a = apply_rows(lambda k: rep[k, near], [points[d * COMPS + c, near] for c in range(3)])
    b = apply_rows(lambda k: rep[k, far], [points[d * COMPS + 3 + c, near] for c in range(3)])
    error = squared(a, b)
    errors[d, near] = error
    for c in range(3):
        here_out[3 * d + c, near] = a[c]
        there_out[3 * d + c, near] = b[c]
    return error


def own_stats(flat, points, rep, errors, mapped, target, blocks, out):
    zero = jnp.zeros((SUB, LANES), jnp.float32)
    top, total, count = zero, zero, zero
    for f in blocks:
        keep = flat.owned(f)
        for d in range(4):
            error = link_values(flat, f, d, points, rep, errors, mapped, target)
            if keep is None:
                continue
            weight = points[d * COMPS + 6, f : f + SUB]
            masked = weight * error
            if keep is not True:
                masked = jnp.where(keep, masked, 0.0)
                weight = jnp.where(keep, weight, 0.0)
            top = jnp.maximum(top, masked)
            total = total + masked
            count = count + weight
    send_stats(out, jnp.max(top), jnp.sum(total), jnp.sum(count))


def first_stats(flat, devices):
    rows = flat.rows

    south_t = 4 * COMPS * flat.span

    def body(points, text, south, rep, errors, mapped, target, out):
        for k in range(12):
            for r in range(rows):
                spread(text[k * rows + r : k * rows + r + 1], rep, k, flat.at(r, -2), flat.span)
            row = south_t + 2 * k
            spread(south[row : row + 1], rep, k, flat.at(rows, -2), flat.span)
        own_stats(flat, points, rep, errors, mapped, target, flat.own_blocks(), out)

    t = flat.tiles
    return call(
        body,
        [(12, t, LANES), (4, t, LANES), (12, t, LANES), (12, t, LANES), (devices, 1, LANES)],
        in_vmem=(0, 1, 2),
    )


def outer_values(flat, points, rep, errors, mapped, target, north, south):
    rows, span = flat.rows, flat.span
    slices, north_t = north_slices(flat)
    for n, skip, count, src in slices:
        at = flat.at(skip - 2, -2)
        points[n, at : at + count] = north[src : src + count]
    for n in range(4 * COMPS):
        at = flat.at(rows, -2)
        points[n, at : at + span] = south[n * span : (n + 1) * span]
    for k in range(12):
        for j in range(2):
            row = north_t + 2 * k + j
            spread(north[row : row + 1], rep, k, flat.at(j - 2, -2), span)
        row = 4 * COMPS * span + 2 * k + 1
        spread(south[row : row + 1], rep, k, flat.at(rows + 1, -2), span)
    inner = set(flat.own_blocks())
    for f in flat.blocks(-2, -2, rows, flat.cols + 1):
        if f not in inner:
            for d in range(4):
                link_values(flat, f, d, points, rep, errors, mapped, target)


def weigh(blocks, points, errors, weights, scale):
    for f in blocks:
        for d in range(4):
            weights[d, f : f + SUB] = points[d * COMPS + 6, f : f + SUB] * scale / (scale + errors[d, f : f + SUB])


def tile_sums(flat, f, points, mapped, target, weights):
    gram = {}
    cross = {}

    def put(store, key, value):
        store[key] = value if key not in store else store[key] + value

    for d in range(4):
        for end in range(2):
            at = f if end == 0 else f - flat.shift[d]
            rows = slice(at, at + SUB)
            base = d * COMPS + 3 * end
            x = [points[base + c, rows] for c in range(3)]
            other = target if end == 0 else mapped
            weight = weights[d, rows]
            weighted = [weight * v for v in x] + [weight]
            for a, b in GRAM:
                if a == 3:
                    put(gram, (a, b), weighted[b])
                else:
                    put(gram, (a, b), weighted[a] * x[b])
            for c in range(3):
                scaled = weight * other[3 * d + c, rows]
                put(cross, (c, 3), scaled)
                for b in range(3):
                    put(cross, (c, b), scaled * x[b])
    return gram, cross


def solve_small(gram, cross):
    factor = {}
    inverse = {}
    for a in range(4):
        for b in range(a + 1):
            value = gram[a, b]
            for i in range(b):
                value = value - factor[a, i] * factor[b, i]
            if a == b:
                inverse[a] = 1.0 / jnp.sqrt(value)
            else:
                factor[a, b] = value * inverse[b]
    result = []
    for c in range(3):
        forward = []
        for a in range(4):
            value = cross[c, a]
            for i in range(a):
                value = value - factor[a, i] * forward[i]
            forward.append(value * inverse[a])
        backward = [None] * 4
        for a in (3, 2, 1, 0):
            value = forward[a]
            for i in range(a + 1, 4):
                value = value - factor[i, a] * backward[i]
            backward[a] = value * inverse[a]
        result.extend(backward)
    return result


def update(flat, blocks, points, rep, mapped, target, weights, damping):
    group = iota((SUB, LANES), 1) // SUB
    results = []
    for start in range(0, len(blocks), LANES // SUB):
        part = blocks[start : start + LANES // SUB]
        gram, cross, old = {}, {}, {}
        for b, f in enumerate(part):
            keep = group == b

            def place(store, key, value):
                store[key] = value if b == 0 else jnp.where(keep, value, store[key])

            sums = tile_sums(flat, f, points, mapped, target, weights)
            for store, found in zip((gram, cross), sums):
                for key, value in found.items():
                    place(store, key, jnp.broadcast_to(jnp.sum(value, axis=1, keepdims=True), value.shape))
            for k in range(12):
                place(old, (k // 4, k % 4), rep[k, f : f + SUB])
        for a in range(4):
            gram[a, a] = gram[a, a] + damping
        for key, value in old.items():
            cross[key] = cross[key] + damping * value
        results.append((part, solve_small(gram, cross)))
    return results


def replicate(results, out):
    for part, solved in results:
        for k, value in enumerate(solved):
            for b, f in enumerate(part):
                out[k, f : f + SUB] = jnp.broadcast_to(value[:, b * SUB : b * SUB + 1], (SUB, LANES))


def first_update(flat, devices):
    rows, cols = flat.rows, flat.cols

    def body(*refs):
        got, north, south = refs[5:8]
        points, rep, errors, mapped, target, new_rep, out, weights = refs[8:]
        state = (points, rep, errors, mapped, target)
        outer_values(flat, *state, north, south)
        largest, mean_error = read_stats(got)
        scale = 0.25 * largest + 1e-06
        damping = damping_scale * mean_error + 1.0
        weigh(flat.blocks(-2, -2, rows, cols + 1), points, errors, weights, scale)
        blocks = flat.blocks(-1, -1, rows, cols)
        replicate(update(flat, blocks, points, rep, mapped, target, weights, damping), new_rep)
        blocks = flat.blocks(-1, -1, rows - 1, cols)
        own_stats(flat, points, new_rep, errors, mapped, target, blocks, out)

    t = flat.tiles
    return call(
        body,
        [(4 * COMPS, t, LANES)] + [(n, t, LANES) for n in (12, 4, 12, 12, 12)] + [(devices, 1, LANES)],
        [(4, t, LANES)],
        in_vmem=range(8),
        aliases={i: i for i in range(5)},
    )


def take_lanes(lines, at, count):
    pieces = []
    while count:
        n, lane = divmod(at, LANES)
        size = min(count, LANES - lane)
        pieces.append(lines[n][:, lane : lane + size])
        at, count = at + size, count - size
    return pieces[0] if len(pieces) == 1 else jnp.concatenate(pieces, axis=1)


def last_update(flat):
    rows, cols = flat.rows, flat.cols

    def body(got0, got1, points, rep, errors, mapped, target, aligned, stats, weights):
        first, mean0 = read_stats(got0)
        largest, mean_error = read_stats(got1)
        scale = 0.25 * largest + 1e-06
        damping = damping_scale * mean_error + 1.0
        weigh(flat.blocks(-1, -1, rows - 1, cols), points, errors, weights, scale)
        results = update(flat, flat.own_blocks(), points, rep, mapped, target, weights, damping)
        diagonal = iota((SUB, LANES), 0) == lax.rem(iota((SUB, LANES), 1), SUB)
        for k in range(12):
            lines = []
            for part, solved in results:
                lines.append(jnp.sum(jnp.where(diagonal, solved[k], 0.0), axis=0, keepdims=True))
            for r in range(rows):
                at = flat.at(r, 0) - results[0][0][0]
                aligned[k, r : r + 1] = take_lanes(lines, at, cols)
        row = iota((2, 2), 0)
        col = iota((2, 2), 1)
        stats[...] = jnp.where(row == 0, jnp.where(col == 0, first, largest), jnp.where(col == 0, mean0, mean_error))

    t = flat.tiles
    return call(body, [(12, rows, cols), (2, 2)], [(4, t, LANES)], in_vmem=range(7), results=None)


def onward(array, axis, by):
    peers = lax.axis_size(axis)
    return lax.ppermute(array, axis, [(i, i + by) for i in range(peers) if 0 <= i + by < peers])


def everyone(array):
    return lax.all_to_all(array, ("row", "col"), 0, 0)


def on_device(points_here, points_there, outlier_mask, transforms):
    rows, cols = transforms.shape[2:]
    devices = lax.axis_size("row") * lax.axis_size("col")
    flat = Flat(rows, cols)
    points, padded, to_first, to_second = pack_cols(flat)(
        points_here, points_there, outlier_mask, transforms.reshape(12 * rows, cols)
    )
    first_swap = swap(to_first, "col", 0)
    second_swap = swap(to_second, "col", 1)
    points, text, to_down, to_up = pack_rows(flat)(points, padded, first_swap, second_swap)
    south = onward(to_up, "row", -1)
    north = onward(to_down, "row", 1)
    rep, errors, mapped, target, sent = first_stats(flat, devices)(points, text, south)
    got0 = everyone(sent)
    points, _, errors, mapped, target, rep, sent = first_update(flat, devices)(
        points, rep, errors, mapped, target, got0, north, south
    )
    got1 = everyone(sent)
    aligned, stats = last_update(flat)(got0, got1, points, rep, errors, mapped, target)
    return aligned.reshape(3, 4, rows, cols), stats


def solution(mesh):
    return jax.shard_map(
        on_device,
        mesh=mesh,
        in_specs=(
            P(None, None, "row", "col", None),
            P(None, None, "row", "col", None),
            P(None, "row", "col", None),
            P(None, None, "row", "col"),
        ),
        out_specs=(P(None, None, "row", "col"), P()),
        check_vma=False,
    )
```

```python
import jax
import jax.numpy as jnp
from jax import lax
from jax.experimental import pallas as pl
from jax.experimental.pallas import tpu as pltpu
from jax.sharding import PartitionSpec as P

LANES = 128
SUB = 8
COMPS = 7

link_offsets = ((0, 1), (1, 0), (1, 1), (1, -1))
damping_scale = 64.0
GRAM = [(a, b) for a in range(4) for b in range(a + 1)]


def call(body, out_shapes, scratch=(), in_vmem=(), in_hbm=(), aliases=None, results=pltpu.VMEM):
    shapes = [(results or jax.ShapeDtypeStruct)(s, jnp.float32) for s in out_shapes]
    vmem = pl.BlockSpec(memory_space=pltpu.VMEM)
    hbm = pl.BlockSpec(memory_space=pltpu.HBM)

    def run(*args):
        spaces = {**dict.fromkeys(in_vmem, pltpu.VMEM), **dict.fromkeys(in_hbm, pltpu.HBM)}
        args = [pltpu.with_memory_space_constraint(v, spaces[i]) if i in spaces else v for i, v in enumerate(args)]
        return pl.pallas_call(
            body,
            out_shape=shapes,
            in_specs=[hbm if i in in_hbm else vmem for i in range(len(args))],
            out_specs=[vmem] * len(shapes),
            scratch_shapes=[pltpu.VMEM(s, jnp.float32) if isinstance(s, tuple) else s for s in scratch],
            input_output_aliases=aliases or {},
            compiler_params=pltpu.CompilerParams(vmem_limit_bytes=16 * 1024 * 1024),
        )(*args)

    return run


def iota(shape, axis):
    return lax.broadcasted_iota(jnp.int32, shape, axis)


WEST_LINKS = [(0, d) for d in (0, 2)] + [(1, d) for d in range(4)]
EAST_LINKS = [(0, d) for d in range(4)] + [(1, 3)]


def side_rows(links, rows):
    return [(d, j, c, (n * COMPS + c) * rows) for n, (j, d) in enumerate(links) for c in range(COMPS)]


def side_count(rows):
    return max(len(WEST_LINKS), len(EAST_LINKS)) * COMPS * rows + SUB


def by_parity(axis, body, first, second):
    odd = lax.rem(lax.axis_index(axis), 2)

    @pl.when(odd == 0)
    def _():
        body(first, second)

    @pl.when(odd == 1)
    def _():
        body(second, first)


def swap(array, axis, first):
    peers = lax.axis_size(axis)
    lower = range(first, peers - 1, 2)
    return lax.ppermute(array, axis, [pair for i in lower for pair in ((i, i + 1), (i + 1, i))])


def pack_cols(flat):
    rows, cols = flat.rows, flat.cols
    groups = 12 * rows // SUB

    def body(here_in, there_in, outlier_in, transforms_in, points, padded, first_swap, second_swap, *scratch):
        here, there, outlier, transforms, sems = scratch
        copies = []
        for n, (source, goal) in enumerate(((here_in, here), (there_in, there), (outlier_in, outlier))):
            copies.append([pltpu.make_async_copy(source.at[d], goal.at[d], sems.at[n, d]) for d in range(4)])
        copies.append([pltpu.make_async_copy(transforms_in, transforms, sems.at[3, 0])])
        for d in range(4):
            for n in range(3):
                copies[n][d].start()
        copies[3][0].start()
        grid_rows = rows * lax.axis_size("row")
        grid_cols = cols * lax.axis_size("col")
        row0 = lax.axis_index("row") * rows
        col_ids = lax.axis_index("col") * cols + iota((cols, LANES), 0)
        for d, (dr, dc) in enumerate(link_offsets):
            col_valid = jnp.where((col_ids + dc >= 0) & (col_ids + dc < grid_cols), 1.0, 0.0)
            for n in range(3):
                copies[n][d].wait()
            for r in range(rows):
                own = slice(flat.at(r, 0), flat.at(r, cols))
                row_valid = jnp.where(row0 + r + dr < grid_rows, 1.0, 0.0)
                points[d * COMPS + 6, own] = outlier[d, r].astype(jnp.float32) * (col_valid * row_valid)
                for c in range(3):
                    points[d * COMPS + c, own] = here[d, c, r]
                    points[d * COMPS + 3 + c, own] = there[d, c, r]

        def pack_points(to_east, to_west):
            for out, links, first in ((to_east, WEST_LINKS, cols - 2), (to_west, EAST_LINKS, 0)):
                for d, j, c, at in side_rows(links, rows):
                    for r in range(rows):
                        tile = flat.at(r, first + j)
                        out[at + r : at + r + 1] = points[d * COMPS + c, tile : tile + 1]

        by_parity("col", pack_points, first_swap, second_swap)
        padded[...] = jnp.zeros((12 * rows, LANES), jnp.float32)
        copies[3][0].wait()
        padded[:, 2 : cols + 2] = transforms[...]
        lane = iota((SUB, LANES), 1)
        packed = []
        for first in (cols - 2, 0):
            value = jnp.zeros((SUB, LANES), jnp.float32)
            for g in range(groups):
                moved = pltpu.roll(padded[g * SUB : (g + 1) * SUB], (2 * g - first - 2) % LANES, 1)
                value = jnp.where((lane == 2 * g) | (lane == 2 * g + 1), moved, value)
            packed.append(value)

        def pack_transforms(to_east, to_west):
            to_east[side_count(rows) - SUB :] = packed[0]
            to_west[side_count(rows) - SUB :] = packed[1]

        by_parity("col", pack_transforms, first_swap, second_swap)

    count = side_count(rows)
    return call(
        body,
        [(4 * COMPS, flat.tiles, LANES), (12 * rows, LANES), (count, LANES), (count, LANES)],
        [
            pltpu.VMEM((4, 3, rows, cols, LANES), jnp.float32),
            pltpu.VMEM((4, 3, rows, cols, LANES), jnp.float32),
            pltpu.VMEM((4, rows, cols, LANES), jnp.int32),
            pltpu.VMEM((12 * rows, cols), jnp.float32),
            pltpu.SemaphoreType.DMA((4, 4)),
        ],
        in_hbm=range(4),
    )


def north_slices(flat):
    span, at, found = flat.span, 0, []
    for d in range(4):
        for c in range(COMPS):
            count = 1 if d == 0 else 2
            found.append((d * COMPS + c, 2 - count, count * span, at))
            at += count * span
    return found, at


def pack_rows(flat):
    rows, cols, span = flat.rows, flat.cols, flat.span
    slices, north_t = north_slices(flat)
    south_t = 4 * COMPS * span

    def body(points_in, padded, first_swap, second_swap, points, text, down, up):
        def unpack(east, west):
            for side, links, first in ((west, WEST_LINKS, -2), (east, EAST_LINKS, cols)):
                for d, j, c, at in side_rows(links, rows):
                    for r in range(rows):
                        tile = flat.at(r, first + j)
                        points[d * COMPS + c, tile : tile + 1] = side[at + r : at + r + 1]
            lane = iota((SUB, LANES), 1)
            from_west = west[side_count(rows) - SUB :]
            from_east = east[side_count(rows) - SUB :]
            for g in range(12 * rows // SUB):
                part = slice(g * SUB, (g + 1) * SUB)
                left = pltpu.roll(from_west, -2 * g % LANES, 1)
                right = pltpu.roll(from_east, (cols + 2 - 2 * g) % LANES, 1)
                value = jnp.where(lane < 2, left, jnp.where(lane < cols + 2, padded[part], right))
                text[part] = jnp.where(lane < span, value, 0.0)

        by_parity("col", unpack, first_swap, second_swap)
        for n in range(4 * COMPS):
            up[n * span : (n + 1) * span] = points[n, flat.at(0, -2) : flat.at(0, -2) + span]
        for k in range(12):
            up[south_t + 2 * k : south_t + 2 * k + 2] = text[k * rows : k * rows + 2]
        for n, skip, count, to in slices:
            at = flat.at(rows - 2 + skip, -2)
            down[to : to + count] = points[n, at : at + count]
        for k in range(12):
            down[north_t + 2 * k : north_t + 2 * k + 2] = text[(k + 1) * rows - 2 : (k + 1) * rows]

    return call(
        body,
        [(4 * COMPS, flat.tiles, LANES), (12 * rows, LANES), (north_t + 24, LANES), (south_t + 24, LANES)],
        in_vmem=(0, 1, 2, 3),
        aliases={0: 0},
    )


def spread(row, out, k, at, span):
    full = -(-span // SUB) * SUB
    wide = jnp.broadcast_to(row, (full, LANES))
    picked = jnp.where(iota((full, LANES), 0) == iota((full, LANES), 1), wide, 0.0)
    value = jnp.broadcast_to(jnp.sum(picked, axis=1, keepdims=True), (full, LANES))
    out[k, at : at + span] = value[:span]


def apply_rows(affine, points):
    mapped = []
    for c in range(3):
        value = affine(4 * c + 3) + affine(4 * c) * points[0]
        value = value + affine(4 * c + 1) * points[1]
        mapped.append(value + affine(4 * c + 2) * points[2])
    return mapped


def squared(here, there):
    delta = [a - b for a, b in zip(here, there)]
    return delta[0] * delta[0] + delta[1] * delta[1] + delta[2] * delta[2]


def send_stats(out, largest, total, count):
    lane = iota(out.shape, len(out.shape) - 1)
    out[...] = jnp.where(lane == 0, largest, jnp.where(lane == 1, total, jnp.where(lane == 2, count, 0.0)))


def read_stats(got):
    values = got[...]
    lane = iota(values.shape, 2)
    largest = jnp.max(jnp.where(lane == 0, values, 0.0))
    total = jnp.sum(jnp.where(lane == 1, values, 0.0))
    count = jnp.sum(jnp.where(lane == 2, values, 0.0))
    return largest, total / jnp.maximum(count, 1.0)


class Flat:

    def __init__(self, rows, cols):
        self.rows, self.cols = rows, cols
        self.span = cols + 4
        self.tiles = -(-((rows + 4) * self.span + self.span + 1) // SUB) * SUB + 2 * SUB
        self.shift = [dr * self.span + dc for dr, dc in link_offsets]

    def at(self, r, c):
        return SUB + (r + 2) * self.span + c + 2

    def blocks(self, r0, c0, r1, c1):
        return range(self.at(r0, c0) // SUB * SUB, self.at(r1, c1) + 1, SUB)

    def own_blocks(self):
        return self.blocks(0, 0, self.rows - 1, self.cols)

    def counted(self, f, d):
        index = iota((SUB, LANES), 0) + f
        keep = None
        for r in range(self.rows):
            dc = link_offsets[d][1] if d >= 2 and r == self.rows - 1 else 0
            low, high = self.at(r, 0 - dc), self.at(r, self.cols - 1 - dc)
            if low <= f and f + SUB - 1 <= high:
                return True
            if low < f + SUB and high >= f:
                one = (index >= low) & (index <= high)
                keep = one if keep is None else keep | one
        return keep


def link_values(flat, f, d, points, rep, errors, here_out, there_out):
    near = slice(f, f + SUB)
    far = slice(f + flat.shift[d], f + flat.shift[d] + SUB)
    a = apply_rows(lambda k: rep[k, near], [points[d * COMPS + c, near] for c in range(3)])
    b = apply_rows(lambda k: rep[k, far], [points[d * COMPS + 3 + c, near] for c in range(3)])
    error = squared(a, b)
    errors[d, near] = error
    for c in range(3):
        here_out[3 * d + c, near] = a[c]
        there_out[3 * d + c, near] = b[c]
    return error


def own_stats(flat, points, rep, errors, mapped, target, blocks, out):
    zero = jnp.zeros((SUB, LANES), jnp.float32)
    top, total, count = zero, zero, zero
    for f in blocks:
        for d in range(4):
            keep = flat.counted(f, d)
            error = link_values(flat, f, d, points, rep, errors, mapped, target)
            if keep is None:
                continue
            weight = points[d * COMPS + 6, f : f + SUB]
            masked = weight * error
            if keep is not True:
                masked = jnp.where(keep, masked, 0.0)
                weight = jnp.where(keep, weight, 0.0)
            top = jnp.maximum(top, masked)
            total = total + masked
            count = count + weight
    send_stats(out, jnp.max(top), jnp.sum(total), jnp.sum(count))


def first_stats(flat, devices):
    rows = flat.rows


    def body(points, text, south, rep, errors, mapped, target, out):
        for k in range(12):
            for r in range(rows):
                spread(text[k * rows + r : k * rows + r + 1], rep, k, flat.at(r, -2), flat.span)
            spread(south[k * rows : k * rows + 1], rep, k, flat.at(rows, -2), flat.span)
        own_stats(flat, points, rep, errors, mapped, target, flat.own_blocks(), out)

    t = flat.tiles
    return call(
        body,
        [(12, t, LANES), (4, t, LANES), (12, t, LANES), (12, t, LANES), (devices, 1, LANES)],
        in_vmem=(0, 1, 2),
    )


def outer_values(flat, points, rep, errors, mapped, target, north, south):
    rows, span = flat.rows, flat.span
    slices, north_t = north_slices(flat)
    for n, skip, count, src in slices:
        at = flat.at(skip - 2, -2)
        points[n, at : at + count] = north[src : src + count]
    for n in range(4 * COMPS):
        at = flat.at(rows, -2)
        points[n, at : at + span] = south[n * span : (n + 1) * span]
    for k in range(12):
        for j in range(2):
            row = north_t + 2 * k + j
            spread(north[row : row + 1], rep, k, flat.at(j - 2, -2), span)
            row = 4 * COMPS * span + 2 * k + j
            spread(south[row : row + 1], rep, k, flat.at(rows + j, -2), span)
    inner = set(f for f in flat.own_blocks() if f + SUB <= flat.at(rows - 1, -2))
    for f in flat.blocks(-2, -2, rows, flat.cols + 1):
        if f not in inner:
            for d in range(4):
                link_values(flat, f, d, points, rep, errors, mapped, target)


def weigh(blocks, points, errors, weights, scale):
    for f in blocks:
        for d in range(4):
            weights[d, f : f + SUB] = points[d * COMPS + 6, f : f + SUB] * scale / (scale + errors[d, f : f + SUB])


def tile_sums(flat, f, points, mapped, target, weights):
    gram = {}
    cross = {}

    def put(store, key, value):
        store[key] = value if key not in store else store[key] + value

    for d in range(4):
        for end in range(2):
            at = f if end == 0 else f - flat.shift[d]
            rows = slice(at, at + SUB)
            base = d * COMPS + 3 * end
            x = [points[base + c, rows] for c in range(3)]
            other = target if end == 0 else mapped
            weight = weights[d, rows]
            weighted = [weight * v for v in x] + [weight]
            for a, b in GRAM:
                if a == 3:
                    put(gram, (a, b), weighted[b])
                else:
                    put(gram, (a, b), weighted[a] * x[b])
            for c in range(3):
                scaled = weight * other[3 * d + c, rows]
                put(cross, (c, 3), scaled)
                for b in range(3):
                    put(cross, (c, b), scaled * x[b])
    return gram, cross


def solve_small(gram, cross):
    factor = {}
    inverse = {}
    for a in range(4):
        for b in range(a + 1):
            value = gram[a, b]
            for i in range(b):
                value = value - factor[a, i] * factor[b, i]
            if a == b:
                inverse[a] = 1.0 / jnp.sqrt(value)
            else:
                factor[a, b] = value * inverse[b]
    result = []
    for c in range(3):
        forward = []
        for a in range(4):
            value = cross[c, a]
            for i in range(a):
                value = value - factor[a, i] * forward[i]
            forward.append(value * inverse[a])
        backward = [None] * 4
        for a in (3, 2, 1, 0):
            value = forward[a]
            for i in range(a + 1, 4):
                value = value - factor[i, a] * backward[i]
            backward[a] = value * inverse[a]
        result.extend(backward)
    return result


def update(flat, blocks, points, rep, mapped, target, weights, damping):
    group = iota((SUB, LANES), 1) // SUB
    results = []
    for start in range(0, len(blocks), LANES // SUB):
        part = blocks[start : start + LANES // SUB]
        gram, cross, old = {}, {}, {}
        for b, f in enumerate(part):
            keep = group == b

            def place(store, key, value):
                store[key] = value if b == 0 else jnp.where(keep, value, store[key])

            sums = tile_sums(flat, f, points, mapped, target, weights)
            for store, found in zip((gram, cross), sums):
                for key, value in found.items():
                    place(store, key, jnp.broadcast_to(jnp.sum(value, axis=1, keepdims=True), value.shape))
            for k in range(12):
                place(old, (k // 4, k % 4), rep[k, f : f + SUB])
        for a in range(4):
            gram[a, a] = gram[a, a] + damping
        for key, value in old.items():
            cross[key] = cross[key] + damping * value
        results.append((part, solve_small(gram, cross)))
    return results


def replicate(results, out):
    for part, solved in results:
        for k, value in enumerate(solved):
            for b, f in enumerate(part):
                out[k, f : f + SUB] = jnp.broadcast_to(value[:, b * SUB : b * SUB + 1], (SUB, LANES))


def first_update(flat, devices):
    rows, cols = flat.rows, flat.cols

    def body(*refs):
        got, north, south = refs[5:8]
        points, rep, errors, mapped, target, new_rep, out, weights = refs[8:]
        state = (points, rep, errors, mapped, target)
        outer_values(flat, *state, north, south)
        largest, mean_error = read_stats(got)
        scale = 0.25 * largest + 1e-06
        damping = damping_scale * mean_error + 1.0
        weigh(flat.blocks(-2, -2, rows, cols + 1), points, errors, weights, scale)
        blocks = flat.blocks(-1, -1, rows, cols)
        replicate(update(flat, blocks, points, rep, mapped, target, weights, damping), new_rep)
        blocks = flat.blocks(-1, -1, rows - 1, cols)
        own_stats(flat, points, new_rep, errors, mapped, target, blocks, out)

    t = flat.tiles
    return call(
        body,
        [(4 * COMPS, t, LANES)] + [(n, t, LANES) for n in (12, 4, 12, 12, 12)] + [(devices, 1, LANES)],
        [(4, t, LANES)],
        in_vmem=range(8),
        aliases={i: i for i in range(5)},
    )


def take_lanes(lines, at, count):
    pieces = []
    while count:
        n, lane = divmod(at, LANES)
        size = min(count, LANES - lane)
        pieces.append(lines[n][:, lane : lane + size])
        at, count = at + size, count - size
    return pieces[0] if len(pieces) == 1 else jnp.concatenate(pieces, axis=1)


def last_update(flat):
    rows, cols = flat.rows, flat.cols

    def body(got0, got1, points, rep, errors, mapped, target, aligned, stats, weights):
        first, mean0 = read_stats(got0)
        largest, mean_error = read_stats(got1)
        scale = 0.25 * largest + 1e-06
        damping = damping_scale * mean_error + 1.0
        weigh(flat.blocks(-1, -1, rows - 1, cols), points, errors, weights, scale)
        results = update(flat, flat.own_blocks(), points, rep, mapped, target, weights, damping)
        diagonal = iota((SUB, LANES), 0) == lax.rem(iota((SUB, LANES), 1), SUB)
        for k in range(12):
            lines = []
            for part, solved in results:
                lines.append(jnp.sum(jnp.where(diagonal, solved[k], 0.0), axis=0, keepdims=True))
            for r in range(rows):
                at = flat.at(r, 0) - results[0][0][0]
                aligned[k, r : r + 1] = take_lanes(lines, at, cols)
        row = iota((2, 2), 0)
        col = iota((2, 2), 1)
        stats[...] = jnp.where(row == 0, jnp.where(col == 0, first, largest), jnp.where(col == 0, mean0, mean_error))

    t = flat.tiles
    return call(body, [(12, rows, cols), (2, 2)], [(4, t, LANES)], in_vmem=range(7), results=None)


def onward(array, axis, by):
    peers = lax.axis_size(axis)
    return lax.ppermute(array, axis, [(i, i + by) for i in range(peers) if 0 <= i + by < peers])


def everyone(array):
    return lax.all_to_all(array, ("row", "col"), 0, 0)


def on_device(points_here, points_there, outlier_mask, transforms):
    rows, cols = transforms.shape[2:]
    devices = lax.axis_size("row") * lax.axis_size("col")
    flat = Flat(rows, cols)
    points, padded, to_first, to_second = pack_cols(flat)(
        points_here, points_there, outlier_mask, transforms.reshape(12 * rows, cols)
    )
    first_swap = swap(to_first, "col", 0)
    second_swap = swap(to_second, "col", 1)
    below = onward(padded, "row", -1)
    points, text, to_down, to_up = pack_rows(flat)(points, padded, first_swap, second_swap)
    south = onward(to_up, "row", -1)
    north = onward(to_down, "row", 1)
    rep, errors, mapped, target, sent = first_stats(flat, devices)(points, text, below)
    got0 = everyone(sent)
    points, _, errors, mapped, target, rep, sent = first_update(flat, devices)(
        points, rep, errors, mapped, target, got0, north, south
    )
    got1 = everyone(sent)
    aligned, stats = last_update(flat)(got0, got1, points, rep, errors, mapped, target)
    return aligned.reshape(3, 4, rows, cols), stats


def solution(mesh):
    return jax.shard_map(
        on_device,
        mesh=mesh,
        in_specs=(
            P(None, None, "row", "col", None),
            P(None, None, "row", "col", None),
            P(None, "row", "col", None),
            P(None, None, "row", "col"),
        ),
        out_specs=(P(None, None, "row", "col"), P()),
        check_vma=False,
    )
```

```python
import jax
import jax.numpy as jnp
from jax import lax
from jax.experimental import pallas as pl
from jax.experimental.pallas import tpu as pltpu
from jax.sharding import PartitionSpec as P

LANES = 128
SUB = 8
COMPS = 7

link_offsets = ((0, 1), (1, 0), (1, 1), (1, -1))
damping_scale = 64.0
GRAM = [(a, b) for a in range(4) for b in range(a + 1)]


def call(body, out_shapes, scratch=(), in_vmem=(), in_hbm=(), aliases=None, results=pltpu.VMEM):
    shapes = [(results or jax.ShapeDtypeStruct)(s, jnp.float32) for s in out_shapes]
    vmem = pl.BlockSpec(memory_space=pltpu.VMEM)
    hbm = pl.BlockSpec(memory_space=pltpu.HBM)

    def run(*args):
        spaces = {**dict.fromkeys(in_vmem, pltpu.VMEM), **dict.fromkeys(in_hbm, pltpu.HBM)}
        args = [pltpu.with_memory_space_constraint(v, spaces[i]) if i in spaces else v for i, v in enumerate(args)]
        return pl.pallas_call(
            body,
            out_shape=shapes,
            in_specs=[hbm if i in in_hbm else vmem for i in range(len(args))],
            out_specs=[vmem] * len(shapes),
            scratch_shapes=[pltpu.VMEM(s, jnp.float32) if isinstance(s, tuple) else s for s in scratch],
            input_output_aliases=aliases or {},
            compiler_params=pltpu.CompilerParams(vmem_limit_bytes=16 * 1024 * 1024),
        )(*args)

    return run


def iota(shape, axis):
    return lax.broadcasted_iota(jnp.int32, shape, axis)


WEST_LINKS = [(0, d) for d in (0, 2)] + [(1, d) for d in range(4)]
EAST_LINKS = [(0, d) for d in range(4)] + [(1, 3)]


def side_rows(links, rows):
    return [(d, j, c, (n * COMPS + c) * rows) for n, (j, d) in enumerate(links) for c in range(COMPS)]


def side_count(rows):
    return max(len(WEST_LINKS), len(EAST_LINKS)) * COMPS * rows + SUB


def by_parity(axis, body, first, second):
    odd = lax.rem(lax.axis_index(axis), 2)

    @pl.when(odd == 0)
    def _():
        body(first, second)

    @pl.when(odd == 1)
    def _():
        body(second, first)


def swap(array, axis, first):
    peers = lax.axis_size(axis)
    lower = range(first, peers - 1, 2)
    return lax.ppermute(array, axis, [pair for i in lower for pair in ((i, i + 1), (i + 1, i))])


def pack_cols(flat):
    rows, cols = flat.rows, flat.cols
    groups = 12 * rows // SUB

    def body(here_in, there_in, outlier_in, transforms_in, points, padded, first_swap, second_swap, far, *scratch):
        here, there, outlier, transforms, sems = scratch
        copies = []
        for n, (source, goal) in enumerate(((here_in, here), (there_in, there), (outlier_in, outlier))):
            copies.append([pltpu.make_async_copy(source.at[d], goal.at[d], sems.at[n, d]) for d in range(4)])
        maps = pltpu.make_async_copy(transforms_in, transforms, sems.at[3, 0])
        maps.start()
        for d in range(4):
            for n in range(3):
                copies[n][d].start()
        padded[...] = jnp.zeros((12 * rows, LANES), jnp.float32)
        maps.wait()
        padded[:, 2 : cols + 2] = transforms[...]
        lane = iota((SUB, LANES), 1)
        packed = []
        for first in (cols - 2, 0):
            value = jnp.zeros((SUB, LANES), jnp.float32)
            for g in range(groups):
                moved = pltpu.roll(padded[g * SUB : (g + 1) * SUB], (2 * g - first - 2) % LANES, 1)
                value = jnp.where((lane == 2 * g) | (lane == 2 * g + 1), moved, value)
            packed.append(value)

        def pack_transforms(to_east, to_west):
            to_east[side_count(rows) - SUB :] = packed[0]
            to_west[side_count(rows) - SUB :] = packed[1]

        by_parity("col", pack_transforms, first_swap, second_swap)
        grid_rows = rows * lax.axis_size("row")
        grid_cols = cols * lax.axis_size("col")
        row0 = lax.axis_index("row") * rows
        col_ids = lax.axis_index("col") * cols + iota((cols, LANES), 0)
        for d, (dr, dc) in enumerate(link_offsets):
            col_valid = jnp.where((col_ids + dc >= 0) & (col_ids + dc < grid_cols), 1.0, 0.0)
            for n in range(3):
                copies[n][d].wait()
            for r in range(rows):
                own = slice(flat.at(r, 0), flat.at(r, cols))
                row_valid = jnp.where(row0 + r + dr < grid_rows, 1.0, 0.0)
                points[d * COMPS + 6, own] = outlier[d, r].astype(jnp.float32) * (col_valid * row_valid)
                for c in range(3):
                    points[d * COMPS + c, own] = here[d, c, r]
                    points[d * COMPS + 3 + c, own] = there[d, c, r]

            def pack_points(to_east, to_west):
                for out, links, first in ((to_east, WEST_LINKS, cols - 2), (to_west, EAST_LINKS, 0)):
                    for link, j, c, at in side_rows(links, rows):
                        for r in range(rows if link == d else 0):
                            tile = flat.at(r, first + j)
                            out[at + r : at + r + 1] = points[d * COMPS + c, tile : tile + 1]

            by_parity("col", pack_points, first_swap, second_swap)
            for c in range(COMPS if d else 0):
                n = (d - 1) * COMPS + c
                far[n * cols : (n + 1) * cols] = points[d * COMPS + c, run_of(flat, rows - 2, 0, cols - 1)]

    count = side_count(rows)
    return call(
        body,
        [
            (4 * COMPS, flat.tiles, LANES),
            (12 * rows, LANES),
            (count, LANES),
            (count, LANES),
            (3 * COMPS * cols, LANES),
        ],
        [
            pltpu.VMEM((4, 3, rows, cols, LANES), jnp.float32),
            pltpu.VMEM((4, 3, rows, cols, LANES), jnp.float32),
            pltpu.VMEM((4, rows, cols, LANES), jnp.int32),
            pltpu.VMEM((12 * rows, cols), jnp.float32),
            pltpu.SemaphoreType.DMA((4, 4)),
        ],
        in_hbm=range(4),
    )


def row_message(flat):
    last = flat.cols
    near = {0: (-2, last), 1: (-1, last), 2: (-2, last), 3: (-1, last + 1)}
    down = [(d, -1) + near[d] for d in range(4)]
    down += [(1, -2, -1, -1), (1, -2, last, last), (2, -2, -2, -1), (3, -2, last, last + 1)]
    up = [(d, flat.rows, -2 if d == 0 else -1, last) for d in range(4)]
    lists, most = [], 0
    for runs in (down, up):
        found, at = [], 0
        for d, r, c0, c1 in runs:
            for c in range(COMPS):
                found.append((d * COMPS + c, r, c0, c1, at))
                at += c1 - c0 + 1
        lists.append(found)
        most = max(most, at)
    return lists[0], lists[1], -(-most // SUB) * SUB


def run_of(flat, r, c0, c1):
    return slice(flat.at(r, c0), flat.at(r, c1) + 1)


def pack_rows(flat):
    rows, cols, span = flat.rows, flat.cols, flat.span
    down, up, maps = row_message(flat)

    def body(points_in, padded, first_swap, second_swap, points, text, first_row, second_row):
        def unpack(east, west):
            for side, links, first in ((west, WEST_LINKS, -2), (east, EAST_LINKS, cols)):
                for d, j, c, at in side_rows(links, rows):
                    for r in range(rows):
                        tile = flat.at(r, first + j)
                        points[d * COMPS + c, tile : tile + 1] = side[at + r : at + r + 1]
            lane = iota((SUB, LANES), 1)
            from_west = west[side_count(rows) - SUB :]
            from_east = east[side_count(rows) - SUB :]
            for g in range(12 * rows // SUB):
                part = slice(g * SUB, (g + 1) * SUB)
                left = pltpu.roll(from_west, -2 * g % LANES, 1)
                right = pltpu.roll(from_east, (cols + 2 - 2 * g) % LANES, 1)
                value = jnp.where(lane < 2, left, jnp.where(lane < cols + 2, padded[part], right))
                text[part] = jnp.where(lane < span, value, 0.0)

        by_parity("col", unpack, first_swap, second_swap)

        def pack(to_south, to_north):
            for out, runs, move, source in ((to_south, down, rows, rows - 2), (to_north, up, -rows, 0)):
                for n, r, c0, c1, at in runs:
                    out[at : at + c1 - c0 + 1] = points[n, run_of(flat, r + move, c0, c1)]
                for k in range(12):
                    row = k * rows + source
                    out[maps + 2 * k : maps + 2 * k + 2] = text[row : row + 2]

        by_parity("row", pack, first_row, second_row)

    return call(
        body,
        [(4 * COMPS, flat.tiles, LANES), (12 * rows, LANES), (maps + 24, LANES), (maps + 24, LANES)],
        in_vmem=(0, 1, 2, 3),
        aliases={0: 0},
    )


def spread(row, out, k, at, span):
    full = -(-span // SUB) * SUB
    wide = jnp.broadcast_to(row, (full, LANES))
    picked = jnp.where(iota((full, LANES), 0) == iota((full, LANES), 1), wide, 0.0)
    value = jnp.broadcast_to(jnp.sum(picked, axis=1, keepdims=True), (full, LANES))
    out[k, at : at + span] = value[:span]


def apply_rows(affine, points):
    mapped = []
    for c in range(3):
        value = affine(4 * c + 3) + affine(4 * c) * points[0]
        value = value + affine(4 * c + 1) * points[1]
        mapped.append(value + affine(4 * c + 2) * points[2])
    return mapped


def squared(here, there):
    delta = [a - b for a, b in zip(here, there)]
    return delta[0] * delta[0] + delta[1] * delta[1] + delta[2] * delta[2]


def send_stats(out, largest, total, count):
    lane = iota(out.shape, len(out.shape) - 1)
    out[...] = jnp.where(lane == 0, largest, jnp.where(lane == 1, total, jnp.where(lane == 2, count, 0.0)))


def read_stats(got):
    values = got[...]
    lane = iota(values.shape, 2)
    largest = jnp.max(jnp.where(lane == 0, values, 0.0))
    total = jnp.sum(jnp.where(lane == 1, values, 0.0))
    count = jnp.sum(jnp.where(lane == 2, values, 0.0))
    return largest, total / jnp.maximum(count, 1.0)


class Flat:

    def __init__(self, rows, cols):
        self.rows, self.cols = rows, cols
        self.span = cols + 4
        self.tiles = -(-((rows + 4) * self.span + self.span + 1) // SUB) * SUB + 2 * SUB
        self.shift = [dr * self.span + dc for dr, dc in link_offsets]

    def at(self, r, c):
        return SUB + (r + 2) * self.span + c + 2

    def blocks(self, r0, c0, r1, c1):
        return range(self.at(r0, c0) // SUB * SUB, self.at(r1, c1) + 1, SUB)

    def own_blocks(self):
        return self.blocks(0, 0, self.rows - 1, self.cols)

    def counted(self, f, d):
        index = iota((SUB, LANES), 0) + f
        keep = None
        for r in range(self.rows):
            dc = link_offsets[d][1] if d >= 2 and r == self.rows - 1 else 0
            low, high = self.at(r, 0 - dc), self.at(r, self.cols - 1 - dc)
            if low <= f and f + SUB - 1 <= high:
                return True
            if low < f + SUB and high >= f:
                one = (index >= low) & (index <= high)
                keep = one if keep is None else keep | one
        return keep


def link_values(flat, f, d, points, rep, errors, here_out, there_out):
    near = slice(f, f + SUB)
    far = slice(f + flat.shift[d], f + flat.shift[d] + SUB)
    a = apply_rows(lambda k: rep[k, near], [points[d * COMPS + c, near] for c in range(3)])
    b = apply_rows(lambda k: rep[k, far], [points[d * COMPS + 3 + c, near] for c in range(3)])
    error = squared(a, b)
    errors[d, near] = error
    for c in range(3):
        here_out[3 * d + c, near] = a[c]
        there_out[3 * d + c, near] = b[c]
    return error


def own_stats(flat, points, rep, errors, mapped, target, blocks, out):
    zero = jnp.zeros((SUB, LANES), jnp.float32)
    top, total, count = zero, zero, zero
    for f in blocks:
        for d in range(4):
            keep = flat.counted(f, d)
            error = link_values(flat, f, d, points, rep, errors, mapped, target)
            if keep is None:
                continue
            weight = points[d * COMPS + 6, f : f + SUB]
            masked = weight * error
            if keep is not True:
                masked = jnp.where(keep, masked, 0.0)
                weight = jnp.where(keep, weight, 0.0)
            top = jnp.maximum(top, masked)
            total = total + masked
            count = count + weight
    send_stats(out, jnp.max(top), jnp.sum(total), jnp.sum(count))


def first_stats(flat, devices):
    rows = flat.rows


    def body(points, text, south, rep, errors, mapped, target, out):
        for k in range(12):
            for r in range(rows):
                spread(text[k * rows + r : k * rows + r + 1], rep, k, flat.at(r, -2), flat.span)
            spread(south[k * rows : k * rows + 1], rep, k, flat.at(rows, -2), flat.span)
        own_stats(flat, points, rep, errors, mapped, target, flat.own_blocks(), out)

    t = flat.tiles
    return call(
        body,
        [(12, t, LANES), (4, t, LANES), (12, t, LANES), (12, t, LANES), (devices, 1, LANES)],
        in_vmem=(0, 1, 2),
    )


def outer_values(flat, points, rep, errors, mapped, target, far, first_row, second_row):
    rows, cols, span = flat.rows, flat.cols, flat.span
    down, up, maps = row_message(flat)
    for n in range(3 * COMPS):
        points[COMPS + n, run_of(flat, -2, 0, cols - 1)] = far[n * cols : (n + 1) * cols]

    def unpack(south, north):
        for source, runs, first in ((north, down, -2), (south, up, rows)):
            for n, r, c0, c1, at in runs:
                points[n, run_of(flat, r, c0, c1)] = source[at : at + c1 - c0 + 1]
            for k in range(12):
                for j in range(2):
                    row = maps + 2 * k + j
                    spread(source[row : row + 1], rep, k, flat.at(first + j, -2), span)

    by_parity("row", unpack, first_row, second_row)
    inner = set(f for f in flat.own_blocks() if f + SUB <= flat.at(rows - 1, -2))
    for f in flat.blocks(-2, -2, rows, flat.cols + 1):
        if f not in inner:
            for d in range(4):
                link_values(flat, f, d, points, rep, errors, mapped, target)


def weigh(blocks, points, errors, weights, scale):
    for f in blocks:
        for d in range(4):
            weights[d, f : f + SUB] = points[d * COMPS + 6, f : f + SUB] * scale / (scale + errors[d, f : f + SUB])


def tile_sums(flat, f, points, mapped, target, weights):
    gram = {}
    cross = {}

    def put(store, key, value):
        store[key] = value if key not in store else store[key] + value

    for d in range(4):
        for end in range(2):
            at = f if end == 0 else f - flat.shift[d]
            rows = slice(at, at + SUB)
            base = d * COMPS + 3 * end
            x = [points[base + c, rows] for c in range(3)]
            other = target if end == 0 else mapped
            weight = weights[d, rows]
            weighted = [weight * v for v in x] + [weight]
            for a, b in GRAM:
                if a == 3:
                    put(gram, (a, b), weighted[b])
                else:
                    put(gram, (a, b), weighted[a] * x[b])
            for c in range(3):
                scaled = weight * other[3 * d + c, rows]
                put(cross, (c, 3), scaled)
                for b in range(3):
                    put(cross, (c, b), scaled * x[b])
    return gram, cross


def solve_small(gram, cross):
    factor = {}
    inverse = {}
    for a in range(4):
        for b in range(a + 1):
            value = gram[a, b]
            for i in range(b):
                value = value - factor[a, i] * factor[b, i]
            if a == b:
                inverse[a] = 1.0 / jnp.sqrt(value)
            else:
                factor[a, b] = value * inverse[b]
    result = []
    for c in range(3):
        forward = []
        for a in range(4):
            value = cross[c, a]
            for i in range(a):
                value = value - factor[a, i] * forward[i]
            forward.append(value * inverse[a])
        backward = [None] * 4
        for a in (3, 2, 1, 0):
            value = forward[a]
            for i in range(a + 1, 4):
                value = value - factor[i, a] * backward[i]
            backward[a] = value * inverse[a]
        result.extend(backward)
    return result


def update(flat, blocks, points, rep, mapped, target, weights, damping):
    group = iota((SUB, LANES), 1) // SUB
    results = []
    for start in range(0, len(blocks), LANES // SUB):
        part = blocks[start : start + LANES // SUB]
        gram, cross, old = {}, {}, {}
        for b, f in enumerate(part):
            keep = group == b

            def place(store, key, value):
                store[key] = value if b == 0 else jnp.where(keep, value, store[key])

            sums = tile_sums(flat, f, points, mapped, target, weights)
            for store, found in zip((gram, cross), sums):
                for key, value in found.items():
                    place(store, key, jnp.broadcast_to(jnp.sum(value, axis=1, keepdims=True), value.shape))
            for k in range(12):
                place(old, (k // 4, k % 4), rep[k, f : f + SUB])
        for a in range(4):
            gram[a, a] = gram[a, a] + damping
        for key, value in old.items():
            cross[key] = cross[key] + damping * value
        results.append((part, solve_small(gram, cross)))
    return results


def replicate(results, out):
    for part, solved in results:
        for k, value in enumerate(solved):
            for b, f in enumerate(part):
                out[k, f : f + SUB] = jnp.broadcast_to(value[:, b * SUB : b * SUB + 1], (SUB, LANES))


def first_update(flat, devices):
    rows, cols = flat.rows, flat.cols

    def body(*refs):
        got, far, first_row, second_row = refs[5:9]
        points, rep, errors, mapped, target, new_rep, out, weights = refs[9:]
        state = (points, rep, errors, mapped, target)
        outer_values(flat, *state, far, first_row, second_row)
        largest, mean_error = read_stats(got)
        scale = 0.25 * largest + 1e-06
        damping = damping_scale * mean_error + 1.0
        weigh(flat.blocks(-2, -2, rows, cols + 1), points, errors, weights, scale)
        blocks = flat.blocks(-1, -1, rows, cols)
        replicate(update(flat, blocks, points, rep, mapped, target, weights, damping), new_rep)
        blocks = flat.blocks(-1, -1, rows - 1, cols)
        own_stats(flat, points, new_rep, errors, mapped, target, blocks, out)

    t = flat.tiles
    return call(
        body,
        [(4 * COMPS, t, LANES)] + [(n, t, LANES) for n in (12, 4, 12, 12, 12)] + [(devices, 1, LANES)],
        [(4, t, LANES)],
        in_vmem=range(9),
        aliases={i: i for i in range(5)},
    )


def take_lanes(lines, at, count):
    pieces = []
    while count:
        n, lane = divmod(at, LANES)
        size = min(count, LANES - lane)
        pieces.append(lines[n][:, lane : lane + size])
        at, count = at + size, count - size
    return pieces[0] if len(pieces) == 1 else jnp.concatenate(pieces, axis=1)


def last_update(flat):
    rows, cols = flat.rows, flat.cols

    def body(got0, got1, points, rep, errors, mapped, target, aligned, stats, weights):
        first, mean0 = read_stats(got0)
        largest, mean_error = read_stats(got1)
        scale = 0.25 * largest + 1e-06
        damping = damping_scale * mean_error + 1.0
        weigh(flat.blocks(-1, -1, rows - 1, cols), points, errors, weights, scale)
        results = update(flat, flat.own_blocks(), points, rep, mapped, target, weights, damping)
        diagonal = iota((SUB, LANES), 0) == lax.rem(iota((SUB, LANES), 1), SUB)
        for k in range(12):
            lines = []
            for part, solved in results:
                lines.append(jnp.sum(jnp.where(diagonal, solved[k], 0.0), axis=0, keepdims=True))
            for r in range(rows):
                at = flat.at(r, 0) - results[0][0][0]
                aligned[k, r : r + 1] = take_lanes(lines, at, cols)
        row = iota((2, 2), 0)
        col = iota((2, 2), 1)
        stats[...] = jnp.where(row == 0, jnp.where(col == 0, first, largest), jnp.where(col == 0, mean0, mean_error))

    t = flat.tiles
    return call(body, [(12, rows, cols), (2, 2)], [(4, t, LANES)], in_vmem=range(7), results=None)


def onward(array, axis, by):
    peers = lax.axis_size(axis)
    return lax.ppermute(array, axis, [(i, i + by) for i in range(peers) if 0 <= i + by < peers])


def everyone(array):
    return lax.all_to_all(array, ("row", "col"), 0, 0)


def on_device(points_here, points_there, outlier_mask, transforms):
    rows, cols = transforms.shape[2:]
    devices = lax.axis_size("row") * lax.axis_size("col")
    flat = Flat(rows, cols)
    points, padded, to_first, to_second, to_far = pack_cols(flat)(
        points_here, points_there, outlier_mask, transforms.reshape(12 * rows, cols)
    )
    first_swap = swap(to_first, "col", 0)
    second_swap = swap(to_second, "col", 1)
    below = onward(padded, "row", -1)
    far = onward(to_far, "row", 1)
    points, text, to_first, to_second = pack_rows(flat)(points, padded, first_swap, second_swap)
    first_row = swap(to_first, "row", 0)
    second_row = swap(to_second, "row", 1)
    rep, errors, mapped, target, sent = first_stats(flat, devices)(points, text, below)
    got0 = everyone(sent)
    points, _, errors, mapped, target, rep, sent = first_update(flat, devices)(
        points, rep, errors, mapped, target, got0, far, first_row, second_row
    )
    got1 = everyone(sent)
    aligned, stats = last_update(flat)(got0, got1, points, rep, errors, mapped, target)
    return aligned.reshape(3, 4, rows, cols), stats


def solution(mesh):
    return jax.shard_map(
        on_device,
        mesh=mesh,
        in_specs=(
            P(None, None, "row", "col", None),
            P(None, None, "row", "col", None),
            P(None, "row", "col", None),
            P(None, None, "row", "col"),
        ),
        out_specs=(P(None, None, "row", "col"), P()),
        check_vma=False,
    )
```

```python
import jax
import jax.numpy as jnp
from jax import lax
from jax.experimental import pallas as pl
from jax.experimental.pallas import tpu as pltpu
from jax.sharding import PartitionSpec as P

LANES = 128
SUB = 8
COMPS = 7

link_offsets = ((0, 1), (1, 0), (1, 1), (1, -1))
damping_scale = 64.0
GRAM = [(a, b) for a in range(4) for b in range(a + 1)]


def call(body, out_shapes, scratch=(), in_vmem=(), in_hbm=(), aliases=None, results=pltpu.VMEM):
    shapes = [(results or jax.ShapeDtypeStruct)(s, jnp.float32) for s in out_shapes]
    vmem = pl.BlockSpec(memory_space=pltpu.VMEM)
    hbm = pl.BlockSpec(memory_space=pltpu.HBM)

    def run(*args):
        spaces = {**dict.fromkeys(in_vmem, pltpu.VMEM), **dict.fromkeys(in_hbm, pltpu.HBM)}
        args = [pltpu.with_memory_space_constraint(v, spaces[i]) if i in spaces else v for i, v in enumerate(args)]
        return pl.pallas_call(
            body,
            out_shape=shapes,
            in_specs=[hbm if i in in_hbm else vmem for i in range(len(args))],
            out_specs=[vmem] * len(shapes),
            scratch_shapes=[pltpu.VMEM(s, jnp.float32) if isinstance(s, tuple) else s for s in scratch],
            input_output_aliases=aliases or {},
            compiler_params=pltpu.CompilerParams(vmem_limit_bytes=16 * 1024 * 1024),
        )(*args)

    return run


def iota(shape, axis):
    return lax.broadcasted_iota(jnp.int32, shape, axis)


WEST_LINKS = [(0, d) for d in (0, 2)] + [(1, d) for d in range(4)]
EAST_LINKS = [(0, d) for d in range(4)] + [(1, 3)]


def side_rows(links, rows):
    return [(d, j, c, (n * COMPS + c) * rows) for n, (j, d) in enumerate(links) for c in range(COMPS)]


def side_count(rows):
    return max(len(WEST_LINKS), len(EAST_LINKS)) * COMPS * rows + SUB


def by_parity(axis, body, first, second):
    odd = lax.rem(lax.axis_index(axis), 2)

    @pl.when(odd == 0)
    def _():
        body(first, second)

    @pl.when(odd == 1)
    def _():
        body(second, first)


def swap(array, axis, first):
    peers = lax.axis_size(axis)
    lower = range(first, peers - 1, 2)
    return lax.ppermute(array, axis, [pair for i in lower for pair in ((i, i + 1), (i + 1, i))])


def pack_cols(flat):
    rows, cols = flat.rows, flat.cols
    groups = 12 * rows // SUB

    def body(here_in, there_in, outlier_in, transforms_in, points, padded, first_swap, second_swap, far, *scratch):
        here, there, outlier, transforms, sems = scratch
        copies = []
        for n, (source, goal) in enumerate(((here_in, here), (there_in, there), (outlier_in, outlier))):
            copies.append([pltpu.make_async_copy(source.at[d], goal.at[d], sems.at[n, d]) for d in range(4)])
        maps = pltpu.make_async_copy(transforms_in, transforms, sems.at[3, 0])
        maps.start()
        for d in range(4):
            for n in range(3):
                copies[n][d].start()
        padded[...] = jnp.zeros((12 * rows, LANES), jnp.float32)
        maps.wait()
        padded[:, 2 : cols + 2] = transforms[...]
        lane = iota((SUB, LANES), 1)
        packed = []
        for first in (cols - 2, 0):
            value = jnp.zeros((SUB, LANES), jnp.float32)
            for g in range(groups):
                moved = pltpu.roll(padded[g * SUB : (g + 1) * SUB], (2 * g - first - 2) % LANES, 1)
                value = jnp.where((lane == 2 * g) | (lane == 2 * g + 1), moved, value)
            packed.append(value)

        def pack_transforms(to_east, to_west):
            to_east[side_count(rows) - SUB :] = packed[0]
            to_west[side_count(rows) - SUB :] = packed[1]

        by_parity("col", pack_transforms, first_swap, second_swap)
        grid_rows = rows * lax.axis_size("row")
        grid_cols = cols * lax.axis_size("col")
        row0 = lax.axis_index("row") * rows
        col_ids = lax.axis_index("col") * cols + iota((cols, LANES), 0)
        for d, (dr, dc) in enumerate(link_offsets):
            col_valid = jnp.where((col_ids + dc >= 0) & (col_ids + dc < grid_cols), 1.0, 0.0)
            for n in range(3):
                copies[n][d].wait()
            for r in range(rows):
                own = slice(flat.at(r, 0), flat.at(r, cols))
                row_valid = jnp.where(row0 + r + dr < grid_rows, 1.0, 0.0)
                points[d * COMPS + 6, own] = outlier[d, r].astype(jnp.float32) * (col_valid * row_valid)
                for c in range(3):
                    points[d * COMPS + c, own] = here[d, c, r]
                    points[d * COMPS + 3 + c, own] = there[d, c, r]

            def pack_points(to_east, to_west):
                for out, links, first in ((to_east, WEST_LINKS, cols - 2), (to_west, EAST_LINKS, 0)):
                    for link, j, c, at in side_rows(links, rows):
                        for r in range(rows if link == d else 0):
                            tile = flat.at(r, first + j)
                            out[at + r : at + r + 1] = points[d * COMPS + c, tile : tile + 1]

            by_parity("col", pack_points, first_swap, second_swap)
            for c in range(COMPS if d else 0):
                n = (d - 1) * COMPS + c
                far[n * cols : (n + 1) * cols] = points[d * COMPS + c, run_of(flat, rows - 2, 0, cols - 1)]

    count = side_count(rows)
    return call(
        body,
        [
            (4 * COMPS, flat.tiles, LANES),
            (12 * rows, LANES),
            (count, LANES),
            (count, LANES),
            (3 * COMPS * cols, LANES),
        ],
        [
            pltpu.VMEM((4, 3, rows, cols, LANES), jnp.float32),
            pltpu.VMEM((4, 3, rows, cols, LANES), jnp.float32),
            pltpu.VMEM((4, rows, cols, LANES), jnp.int32),
            pltpu.VMEM((12 * rows, cols), jnp.float32),
            pltpu.SemaphoreType.DMA((4, 4)),
        ],
        in_hbm=range(4),
    )


def row_message(flat):
    last = flat.cols
    near = {0: (-2, last), 1: (-1, last), 2: (-2, last), 3: (-1, last + 1)}
    down = [(d, -1) + near[d] for d in range(4)]
    down += [(1, -2, -1, -1), (1, -2, last, last), (2, -2, -2, -1), (3, -2, last, last + 1)]
    up = [(d, flat.rows, -2 if d == 0 else -1, last) for d in range(4)]
    lists, most = [], 0
    for runs in (down, up):
        found, at = [], 0
        for d, r, c0, c1 in runs:
            for c in range(COMPS):
                found.append((d * COMPS + c, r, c0, c1, at))
                at += c1 - c0 + 1
        lists.append(found)
        most = max(most, at)
    return lists[0], lists[1], -(-most // SUB) * SUB


def run_of(flat, r, c0, c1):
    return slice(flat.at(r, c0), flat.at(r, c1) + 1)


def pack_rows(flat):
    rows, cols, span = flat.rows, flat.cols, flat.span
    down, up, maps = row_message(flat)

    def body(points_in, padded, first_swap, second_swap, points, text, first_row, second_row):
        def unpack(east, west):
            for side, links, first in ((west, WEST_LINKS, -2), (east, EAST_LINKS, cols)):
                for d, j, c, at in side_rows(links, rows):
                    for r in range(rows):
                        tile = flat.at(r, first + j)
                        points[d * COMPS + c, tile : tile + 1] = side[at + r : at + r + 1]
            lane = iota((SUB, LANES), 1)
            from_west = west[side_count(rows) - SUB :]
            from_east = east[side_count(rows) - SUB :]
            for g in range(12 * rows // SUB):
                part = slice(g * SUB, (g + 1) * SUB)
                left = pltpu.roll(from_west, -2 * g % LANES, 1)
                right = pltpu.roll(from_east, (cols + 2 - 2 * g) % LANES, 1)
                value = jnp.where(lane < 2, left, jnp.where(lane < cols + 2, padded[part], right))
                text[part] = jnp.where(lane < span, value, 0.0)

        by_parity("col", unpack, first_swap, second_swap)

        def pack(to_south, to_north):
            for out, runs, move, source in ((to_south, down, rows, rows - 2), (to_north, up, -rows, 0)):
                for n, r, c0, c1, at in runs:
                    out[at : at + c1 - c0 + 1] = points[n, run_of(flat, r + move, c0, c1)]
                for k in range(12):
                    row = k * rows + source
                    out[maps + 2 * k : maps + 2 * k + 2] = text[row : row + 2]

        by_parity("row", pack, first_row, second_row)

    return call(
        body,
        [(4 * COMPS, flat.tiles, LANES), (12 * rows, LANES), (maps + 24, LANES), (maps + 24, LANES)],
        in_vmem=(0, 1, 2, 3),
        aliases={0: 0},
    )


def spread(row, out, k, at, span):
    full = -(-span // SUB) * SUB
    wide = jnp.broadcast_to(row, (full, LANES))
    picked = jnp.where(iota((full, LANES), 0) == iota((full, LANES), 1), wide, 0.0)
    value = jnp.broadcast_to(jnp.sum(picked, axis=1, keepdims=True), (full, LANES))
    out[k, at : at + span] = value[:span]


def apply_rows(affine, points):
    mapped = []
    for c in range(3):
        value = affine(4 * c + 3) + affine(4 * c) * points[0]
        value = value + affine(4 * c + 1) * points[1]
        mapped.append(value + affine(4 * c + 2) * points[2])
    return mapped


def squared(here, there):
    delta = [a - b for a, b in zip(here, there)]
    return delta[0] * delta[0] + delta[1] * delta[1] + delta[2] * delta[2]


def send_stats(out, top, total, count):
    def one(reduce, value):
        value = reduce(reduce(value, axis=0, keepdims=True), axis=1, keepdims=True)
        return jnp.broadcast_to(value, (1, LANES))

    lane = iota((1, LANES), 1)
    value = jnp.where(lane == 1, one(jnp.sum, total), jnp.where(lane == 2, one(jnp.sum, count), 0.0))
    value = jnp.where(lane == 0, one(jnp.max, top), value)
    out[...] = jnp.broadcast_to(value[None], out.shape)


def read_stats(got):
    values = got[...]
    most = jnp.max(values, axis=0)
    sums = jnp.sum(values, axis=0)

    def spread_lane(value, n):
        return jnp.broadcast_to(value[:, n : n + 1], (SUB, LANES))

    return spread_lane(most, 0), spread_lane(sums, 1) / jnp.maximum(spread_lane(sums, 2), 1.0)


class Flat:

    def __init__(self, rows, cols):
        self.rows, self.cols = rows, cols
        self.span = cols + 4
        self.tiles = -(-((rows + 4) * self.span + self.span + 1) // SUB) * SUB + 2 * SUB
        self.shift = [dr * self.span + dc for dr, dc in link_offsets]

    def at(self, r, c):
        return SUB + (r + 2) * self.span + c + 2

    def blocks(self, r0, c0, r1, c1):
        return range(self.at(r0, c0) // SUB * SUB, self.at(r1, c1) + 1, SUB)

    def own_blocks(self):
        return self.blocks(0, 0, self.rows - 1, self.cols)

    def counted(self, f, d):
        index = iota((SUB, LANES), 0) + f
        keep = None
        for r in range(self.rows):
            dc = link_offsets[d][1] if d >= 2 and r == self.rows - 1 else 0
            low, high = self.at(r, 0 - dc), self.at(r, self.cols - 1 - dc)
            if low <= f and f + SUB - 1 <= high:
                return True
            if low < f + SUB and high >= f:
                one = (index >= low) & (index <= high)
                keep = one if keep is None else keep | one
        return keep


def link_values(flat, f, d, points, rep, errors, here_out, there_out):
    near = slice(f, f + SUB)
    far = slice(f + flat.shift[d], f + flat.shift[d] + SUB)
    a = apply_rows(lambda k: rep[k, near], [points[d * COMPS + c, near] for c in range(3)])
    b = apply_rows(lambda k: rep[k, far], [points[d * COMPS + 3 + c, near] for c in range(3)])
    error = squared(a, b)
    errors[d, near] = error
    for c in range(3):
        here_out[3 * d + c, near] = a[c]
        there_out[3 * d + c, near] = b[c]
    return error


def own_stats(flat, points, rep, errors, mapped, target, blocks, out):
    zero = jnp.zeros((SUB, LANES), jnp.float32)
    top, total, count = zero, zero, zero
    for f in blocks:
        for d in range(4):
            keep = flat.counted(f, d)
            error = link_values(flat, f, d, points, rep, errors, mapped, target)
            if keep is None:
                continue
            weight = points[d * COMPS + 6, f : f + SUB]
            masked = weight * error
            if keep is not True:
                masked = jnp.where(keep, masked, 0.0)
                weight = jnp.where(keep, weight, 0.0)
            top = jnp.maximum(top, masked)
            total = total + masked
            count = count + weight
    send_stats(out, top, total, count)


def first_stats(flat, devices):
    rows = flat.rows


    def body(points, text, south, rep, errors, mapped, target, out):
        for k in range(12):
            for r in range(rows):
                spread(text[k * rows + r : k * rows + r + 1], rep, k, flat.at(r, -2), flat.span)
            spread(south[k * rows : k * rows + 1], rep, k, flat.at(rows, -2), flat.span)
        own_stats(flat, points, rep, errors, mapped, target, flat.own_blocks(), out)

    t = flat.tiles
    return call(
        body,
        [(12, t, LANES), (4, t, LANES), (12, t, LANES), (12, t, LANES), (devices, 1, LANES)],
        in_vmem=(0, 1, 2),
    )


def outer_values(flat, points, rep, errors, mapped, target, far, first_row, second_row):
    rows, cols, span = flat.rows, flat.cols, flat.span
    down, up, maps = row_message(flat)
    for n in range(3 * COMPS):
        points[COMPS + n, run_of(flat, -2, 0, cols - 1)] = far[n * cols : (n + 1) * cols]

    def unpack(south, north):
        for source, runs, first in ((north, down, -2), (south, up, rows)):
            for n, r, c0, c1, at in runs:
                points[n, run_of(flat, r, c0, c1)] = source[at : at + c1 - c0 + 1]
            for k in range(12):
                for j in range(2):
                    row = maps + 2 * k + j
                    spread(source[row : row + 1], rep, k, flat.at(first + j, -2), span)

    by_parity("row", unpack, first_row, second_row)
    inner = set(f for f in flat.own_blocks() if f + SUB <= flat.at(rows - 1, -2))
    for f in flat.blocks(-2, -2, rows, flat.cols + 1):
        if f not in inner:
            for d in range(4):
                link_values(flat, f, d, points, rep, errors, mapped, target)


def weigh(blocks, points, errors, weights, scale):
    for f in blocks:
        for d in range(4):
            weights[d, f : f + SUB] = points[d * COMPS + 6, f : f + SUB] * scale / (scale + errors[d, f : f + SUB])


def tile_sums(flat, f, points, mapped, target, weights):
    gram = {}
    cross = {}

    def put(store, key, value):
        store[key] = value if key not in store else store[key] + value

    for d in range(4):
        for end in range(2):
            at = f if end == 0 else f - flat.shift[d]
            rows = slice(at, at + SUB)
            base = d * COMPS + 3 * end
            x = [points[base + c, rows] for c in range(3)]
            other = target if end == 0 else mapped
            weight = weights[d, rows]
            weighted = [weight * v for v in x] + [weight]
            for a, b in GRAM:
                if a == 3:
                    put(gram, (a, b), weighted[b])
                else:
                    put(gram, (a, b), weighted[a] * x[b])
            for c in range(3):
                scaled = weight * other[3 * d + c, rows]
                put(cross, (c, 3), scaled)
                for b in range(3):
                    put(cross, (c, b), scaled * x[b])
    return gram, cross


def solve_small(gram, cross):
    factor = {}
    inverse = {}
    for a in range(4):
        for b in range(a + 1):
            value = gram[a, b]
            for i in range(b):
                value = value - factor[a, i] * factor[b, i]
            if a == b:
                inverse[a] = 1.0 / jnp.sqrt(value)
            else:
                factor[a, b] = value * inverse[b]
    result = []
    for c in range(3):
        forward = []
        for a in range(4):
            value = cross[c, a]
            for i in range(a):
                value = value - factor[a, i] * forward[i]
            forward.append(value * inverse[a])
        backward = [None] * 4
        for a in (3, 2, 1, 0):
            value = forward[a]
            for i in range(a + 1, 4):
                value = value - factor[i, a] * backward[i]
            backward[a] = value * inverse[a]
        result.extend(backward)
    return result


def update(flat, blocks, points, rep, mapped, target, weights, damping):
    group = iota((SUB, LANES), 1) // SUB
    results = []
    for start in range(0, len(blocks), LANES // SUB):
        part = blocks[start : start + LANES // SUB]
        gram, cross, old = {}, {}, {}
        for b, f in enumerate(part):
            keep = group == b

            def place(store, key, value):
                store[key] = value if b == 0 else jnp.where(keep, value, store[key])

            sums = tile_sums(flat, f, points, mapped, target, weights)
            for store, found in zip((gram, cross), sums):
                for key, value in found.items():
                    place(store, key, jnp.broadcast_to(jnp.sum(value, axis=1, keepdims=True), value.shape))
            for k in range(12):
                place(old, (k // 4, k % 4), rep[k, f : f + SUB])
        for a in range(4):
            gram[a, a] = gram[a, a] + damping
        for key, value in old.items():
            cross[key] = cross[key] + damping * value
        results.append((part, solve_small(gram, cross)))
    return results


def replicate(results, out):
    for part, solved in results:
        for k, value in enumerate(solved):
            for b, f in enumerate(part):
                out[k, f : f + SUB] = jnp.broadcast_to(value[:, b * SUB : b * SUB + 1], (SUB, LANES))


def first_update(flat, devices):
    rows, cols = flat.rows, flat.cols

    def body(*refs):
        got, far, first_row, second_row = refs[5:9]
        points, rep, errors, mapped, target, new_rep, out, weights = refs[9:]
        state = (points, rep, errors, mapped, target)
        outer_values(flat, *state, far, first_row, second_row)
        largest, mean_error = read_stats(got)
        scale = 0.25 * largest + 1e-06
        damping = damping_scale * mean_error + 1.0
        weigh(flat.blocks(-2, -2, rows, cols + 1), points, errors, weights, scale)
        blocks = flat.blocks(-1, -1, rows, cols)
        replicate(update(flat, blocks, points, rep, mapped, target, weights, damping), new_rep)
        blocks = flat.blocks(-1, -1, rows - 1, cols)
        own_stats(flat, points, new_rep, errors, mapped, target, blocks, out)

    t = flat.tiles
    return call(
        body,
        [(4 * COMPS, t, LANES)] + [(n, t, LANES) for n in (12, 4, 12, 12, 12)] + [(devices, 1, LANES)],
        [(4, t, LANES)],
        in_vmem=range(9),
        aliases={i: i for i in range(5)},
    )


def take_lanes(lines, at, count):
    pieces = []
    while count:
        n, lane = divmod(at, LANES)
        size = min(count, LANES - lane)
        pieces.append(lines[n][:, lane : lane + size])
        at, count = at + size, count - size
    return pieces[0] if len(pieces) == 1 else jnp.concatenate(pieces, axis=1)


def last_update(flat):
    rows, cols = flat.rows, flat.cols

    def body(got0, got1, points, rep, errors, mapped, target, aligned, stats, weights):
        first, mean0 = read_stats(got0)
        largest, mean_error = read_stats(got1)
        scale = 0.25 * largest + 1e-06
        damping = damping_scale * mean_error + 1.0
        weigh(flat.blocks(-1, -1, rows - 1, cols), points, errors, weights, scale)
        results = update(flat, flat.own_blocks(), points, rep, mapped, target, weights, damping)
        diagonal = iota((SUB, LANES), 0) == lax.rem(iota((SUB, LANES), 1), SUB)
        for k in range(12):
            lines = []
            for part, solved in results:
                lines.append(jnp.sum(jnp.where(diagonal, solved[k], 0.0), axis=0, keepdims=True))
            for r in range(rows):
                at = flat.at(r, 0) - results[0][0][0]
                aligned[k, r : r + 1] = take_lanes(lines, at, cols)
        row = iota((2, 2), 0)
        col = iota((2, 2), 1)
        first, largest, mean0, mean_error = [v[0:2, 0:2] for v in (first, largest, mean0, mean_error)]
        stats[...] = jnp.where(row == 0, jnp.where(col == 0, first, largest), jnp.where(col == 0, mean0, mean_error))

    t = flat.tiles
    return call(body, [(12, rows, cols), (2, 2)], [(4, t, LANES)], in_vmem=range(7), results=None)


def onward(array, axis, by):
    peers = lax.axis_size(axis)
    return lax.ppermute(array, axis, [(i, i + by) for i in range(peers) if 0 <= i + by < peers])


def everyone(array):
    return lax.all_to_all(array, ("row", "col"), 0, 0)


def on_device(points_here, points_there, outlier_mask, transforms):
    rows, cols = transforms.shape[2:]
    devices = lax.axis_size("row") * lax.axis_size("col")
    flat = Flat(rows, cols)
    points, padded, to_first, to_second, to_far = pack_cols(flat)(
        points_here, points_there, outlier_mask, transforms.reshape(12 * rows, cols)
    )
    first_swap = swap(to_first, "col", 0)
    second_swap = swap(to_second, "col", 1)
    below = onward(padded, "row", -1)
    far = onward(to_far, "row", 1)
    points, text, to_first, to_second = pack_rows(flat)(points, padded, first_swap, second_swap)
    first_row = swap(to_first, "row", 0)
    second_row = swap(to_second, "row", 1)
    rep, errors, mapped, target, sent = first_stats(flat, devices)(points, text, below)
    got0 = everyone(sent)
    points, _, errors, mapped, target, rep, sent = first_update(flat, devices)(
        points, rep, errors, mapped, target, got0, far, first_row, second_row
    )
    got1 = everyone(sent)
    aligned, stats = last_update(flat)(got0, got1, points, rep, errors, mapped, target)
    return aligned.reshape(3, 4, rows, cols), stats


def solution(mesh):
    return jax.shard_map(
        on_device,
        mesh=mesh,
        in_specs=(
            P(None, None, "row", "col", None),
            P(None, None, "row", "col", None),
            P(None, "row", "col", None),
            P(None, None, "row", "col"),
        ),
        out_specs=(P(None, None, "row", "col"), P()),
        check_vma=False,
    )
```

```python
import jax
import jax.numpy as jnp
from jax import lax
from jax.experimental import pallas as pl
from jax.experimental.pallas import tpu as pltpu
from jax.sharding import PartitionSpec as P

LANES = 128
SUB = 8
COMPS = 7

link_offsets = ((0, 1), (1, 0), (1, 1), (1, -1))
damping_scale = 64.0
GRAM = [(a, b) for a in range(4) for b in range(a + 1)]


def call(body, out_shapes, scratch=(), in_vmem=(), in_hbm=(), aliases=None, results=pltpu.VMEM):
    shapes = [(results or jax.ShapeDtypeStruct)(s, jnp.float32) for s in out_shapes]
    vmem = pl.BlockSpec(memory_space=pltpu.VMEM)
    hbm = pl.BlockSpec(memory_space=pltpu.HBM)

    def run(*args):
        spaces = {**dict.fromkeys(in_vmem, pltpu.VMEM), **dict.fromkeys(in_hbm, pltpu.HBM)}
        args = [pltpu.with_memory_space_constraint(v, spaces[i]) if i in spaces else v for i, v in enumerate(args)]
        return pl.pallas_call(
            body,
            out_shape=shapes,
            in_specs=[hbm if i in in_hbm else vmem for i in range(len(args))],
            out_specs=[vmem] * len(shapes),
            scratch_shapes=[pltpu.VMEM(s, jnp.float32) if isinstance(s, tuple) else s for s in scratch],
            input_output_aliases=aliases or {},
            compiler_params=pltpu.CompilerParams(vmem_limit_bytes=16 * 1024 * 1024),
        )(*args)

    return run


def iota(shape, axis):
    return lax.broadcasted_iota(jnp.int32, shape, axis)


WEST_LINKS = [(0, d) for d in (0, 2)] + [(1, d) for d in range(4)]
EAST_LINKS = [(0, d) for d in range(4)] + [(1, 3)]


def side_rows(links, rows):
    return [(d, j, c, (n * COMPS + c) * rows) for n, (j, d) in enumerate(links) for c in range(COMPS)]


def side_count(rows):
    return max(len(WEST_LINKS), len(EAST_LINKS)) * COMPS * rows + SUB


def by_parity(axis, body, first, second):
    odd = lax.rem(lax.axis_index(axis), 2)

    @pl.when(odd == 0)
    def _():
        body(first, second)

    @pl.when(odd == 1)
    def _():
        body(second, first)


def swap(array, axis, first):
    peers = lax.axis_size(axis)
    lower = range(first, peers - 1, 2)
    return lax.ppermute(array, axis, [pair for i in lower for pair in ((i, i + 1), (i + 1, i))])


def pack_cols(flat):
    rows, cols = flat.rows, flat.cols
    groups = 12 * rows // SUB

    def body(here_in, there_in, outlier_in, transforms_in, points, padded, first_swap, second_swap, far, *scratch):
        here, there, outlier, transforms, sems = scratch
        copies = []
        for n, (source, goal) in enumerate(((here_in, here), (there_in, there), (outlier_in, outlier))):
            copies.append([pltpu.make_async_copy(source.at[d], goal.at[d], sems.at[n, d]) for d in range(4)])
        maps = pltpu.make_async_copy(transforms_in, transforms, sems.at[3, 0])
        maps.start()
        for d in range(4):
            for n in range(3):
                copies[n][d].start()
        padded[...] = jnp.zeros((12 * rows, LANES), jnp.float32)
        maps.wait()
        padded[:, 2 : cols + 2] = transforms[...]
        lane = iota((SUB, LANES), 1)
        packed = []
        for first in (cols - 2, 0):
            value = jnp.zeros((SUB, LANES), jnp.float32)
            for g in range(groups):
                moved = pltpu.roll(padded[g * SUB : (g + 1) * SUB], (2 * g - first - 2) % LANES, 1)
                value = jnp.where((lane == 2 * g) | (lane == 2 * g + 1), moved, value)
            packed.append(value)

        def pack_transforms(to_east, to_west):
            to_east[side_count(rows) - SUB :] = packed[0]
            to_west[side_count(rows) - SUB :] = packed[1]

        by_parity("col", pack_transforms, first_swap, second_swap)
        grid_rows = rows * lax.axis_size("row")
        grid_cols = cols * lax.axis_size("col")
        row0 = lax.axis_index("row") * rows
        col_ids = lax.axis_index("col") * cols + iota((cols, LANES), 0)
        for d, (dr, dc) in enumerate(link_offsets):
            col_valid = jnp.where((col_ids + dc >= 0) & (col_ids + dc < grid_cols), 1.0, 0.0)
            for n in range(3):
                copies[n][d].wait()
            for r in range(rows):
                own = slice(flat.at(r, 0), flat.at(r, cols))
                row_valid = jnp.where(row0 + r + dr < grid_rows, 1.0, 0.0)
                points[d * COMPS + 6, own] = outlier[d, r].astype(jnp.float32) * (col_valid * row_valid)
                for c in range(3):
                    points[d * COMPS + c, own] = here[d, c, r]
                    points[d * COMPS + 3 + c, own] = there[d, c, r]

            def pack_points(to_east, to_west):
                for out, links, first in ((to_east, WEST_LINKS, cols - 2), (to_west, EAST_LINKS, 0)):
                    for link, j, c, at in side_rows(links, rows):
                        for r in range(rows if link == d else 0):
                            tile = flat.at(r, first + j)
                            out[at + r : at + r + 1] = points[d * COMPS + c, tile : tile + 1]

            by_parity("col", pack_points, first_swap, second_swap)
            for c in range(COMPS if d else 0):
                n = (d - 1) * COMPS + c
                far[n * cols : (n + 1) * cols] = points[d * COMPS + c, run_of(flat, rows - 2, 0, cols - 1)]

    count = side_count(rows)
    return call(
        body,
        [
            (4 * COMPS, flat.tiles, LANES),
            (12 * rows, LANES),
            (count, LANES),
            (count, LANES),
            (3 * COMPS * cols, LANES),
        ],
        [
            pltpu.VMEM((4, 3, rows, cols, LANES), jnp.float32),
            pltpu.VMEM((4, 3, rows, cols, LANES), jnp.float32),
            pltpu.VMEM((4, rows, cols, LANES), jnp.int32),
            pltpu.VMEM((12 * rows, cols), jnp.float32),
            pltpu.SemaphoreType.DMA((4, 4)),
        ],
        in_hbm=range(4),
    )


def row_message(flat):
    last = flat.cols
    near = {0: (-2, last), 1: (-1, last), 2: (-2, last), 3: (-1, last + 1)}
    down = [(d, -1) + near[d] for d in range(4)]
    down += [(1, -2, -1, -1), (1, -2, last, last), (2, -2, -2, -1), (3, -2, last, last + 1)]
    up = [(d, flat.rows, -2 if d == 0 else -1, last) for d in range(4)]
    lists, most = [], 0
    for runs in (down, up):
        found, at = [], 0
        for d, r, c0, c1 in runs:
            for c in range(COMPS):
                found.append((d * COMPS + c, r, c0, c1, at))
                at += c1 - c0 + 1
        lists.append(found)
        most = max(most, at)
    return lists[0], lists[1], -(-most // SUB) * SUB


def run_of(flat, r, c0, c1):
    return slice(flat.at(r, c0), flat.at(r, c1) + 1)


def pack_rows(flat):
    rows, cols, span = flat.rows, flat.cols, flat.span
    down, up, maps = row_message(flat)

    def body(points_in, padded, first_swap, second_swap, points, text, first_row, second_row):
        def unpack(east, west):
            for side, links, first in ((west, WEST_LINKS, -2), (east, EAST_LINKS, cols)):
                for d, j, c, at in side_rows(links, rows):
                    for r in range(rows):
                        tile = flat.at(r, first + j)
                        points[d * COMPS + c, tile : tile + 1] = side[at + r : at + r + 1]
            lane = iota((SUB, LANES), 1)
            from_west = west[side_count(rows) - SUB :]
            from_east = east[side_count(rows) - SUB :]
            for g in range(12 * rows // SUB):
                part = slice(g * SUB, (g + 1) * SUB)
                left = pltpu.roll(from_west, -2 * g % LANES, 1)
                right = pltpu.roll(from_east, (cols + 2 - 2 * g) % LANES, 1)
                value = jnp.where(lane < 2, left, jnp.where(lane < cols + 2, padded[part], right))
                text[part] = jnp.where(lane < span, value, 0.0)

        by_parity("col", unpack, first_swap, second_swap)

        def pack(to_south, to_north):
            for out, runs, move, source in ((to_south, down, rows, rows - 2), (to_north, up, -rows, 0)):
                for n, r, c0, c1, at in runs:
                    out[at : at + c1 - c0 + 1] = points[n, run_of(flat, r + move, c0, c1)]
                for k in range(12):
                    row = k * rows + source
                    out[maps + 2 * k : maps + 2 * k + 2] = text[row : row + 2]

        by_parity("row", pack, first_row, second_row)

    return call(
        body,
        [(4 * COMPS, flat.tiles, LANES), (12 * rows, LANES), (maps + 24, LANES), (maps + 24, LANES)],
        in_vmem=(0, 1, 2, 3),
        aliases={0: 0},
    )


def spread(row, out, k, at, span):
    full = -(-span // SUB) * SUB
    wide = jnp.broadcast_to(row, (full, LANES))
    picked = jnp.where(iota((full, LANES), 0) == iota((full, LANES), 1), wide, 0.0)
    value = jnp.broadcast_to(jnp.sum(picked, axis=1, keepdims=True), (full, LANES))
    out[k, at : at + span] = value[:span]


def apply_rows(affine, points):
    mapped = []
    for c in range(3):
        value = affine(4 * c + 3) + affine(4 * c) * points[0]
        value = value + affine(4 * c + 1) * points[1]
        mapped.append(value + affine(4 * c + 2) * points[2])
    return mapped


def squared(here, there):
    delta = [a - b for a, b in zip(here, there)]
    return delta[0] * delta[0] + delta[1] * delta[1] + delta[2] * delta[2]


def send_stats(out, top, total, count):
    def one(reduce, value):
        value = reduce(reduce(value, axis=0, keepdims=True), axis=1, keepdims=True)
        return jnp.broadcast_to(value, (1, LANES))

    lane = iota((1, LANES), 1)
    value = jnp.where(lane == 1, one(jnp.sum, total), jnp.where(lane == 2, one(jnp.sum, count), 0.0))
    value = jnp.where(lane == 0, one(jnp.max, top), value)
    out[...] = jnp.broadcast_to(value[None], out.shape)


def read_stats(got):
    values = got[...]
    most = jnp.max(values, axis=0)
    sums = jnp.sum(values, axis=0)

    def spread_lane(value, n):
        return jnp.broadcast_to(value[:, n : n + 1], (SUB, LANES))

    return spread_lane(most, 0), spread_lane(sums, 1) / jnp.maximum(spread_lane(sums, 2), 1.0)


class Flat:

    def __init__(self, rows, cols):
        self.rows, self.cols = rows, cols
        self.span = cols + 4
        self.tiles = -(-((rows + 4) * self.span + self.span + 1) // SUB) * SUB + 2 * SUB
        self.shift = [dr * self.span + dc for dr, dc in link_offsets]

    def at(self, r, c):
        return SUB + (r + 2) * self.span + c + 2

    def blocks(self, r0, c0, r1, c1):
        return range(self.at(r0, c0) // SUB * SUB, self.at(r1, c1) + 1, SUB)

    def own_blocks(self):
        return self.blocks(0, 0, self.rows - 1, self.cols)

    def counted(self, f, d):
        index = iota((SUB, LANES), 0) + f
        keep = None
        for r in range(self.rows):
            dc = link_offsets[d][1] if d >= 2 and r == self.rows - 1 else 0
            low, high = self.at(r, 0 - dc), self.at(r, self.cols - 1 - dc)
            if low <= f and f + SUB - 1 <= high:
                return True
            if low < f + SUB and high >= f:
                one = (index >= low) & (index <= high)
                keep = one if keep is None else keep | one
        return keep


def link_values(flat, f, d, points, rep, errors, here_out, there_out):
    near = slice(f, f + SUB)
    far = slice(f + flat.shift[d], f + flat.shift[d] + SUB)
    a = apply_rows(lambda k: rep[k, near], [points[d * COMPS + c, near] for c in range(3)])
    b = apply_rows(lambda k: rep[k, far], [points[d * COMPS + 3 + c, near] for c in range(3)])
    error = squared(a, b)
    errors[d, near] = error
    for c in range(3):
        here_out[3 * d + c, near] = a[c]
        there_out[3 * d + c, near] = b[c]
    return error


def own_stats(flat, points, rep, errors, mapped, target, blocks, out):
    zero = jnp.zeros((SUB, LANES), jnp.float32)
    top, total, count = zero, zero, zero
    for f in blocks:
        for d in range(4):
            keep = flat.counted(f, d)
            error = link_values(flat, f, d, points, rep, errors, mapped, target)
            if keep is None:
                continue
            weight = points[d * COMPS + 6, f : f + SUB]
            masked = weight * error
            if keep is not True:
                masked = jnp.where(keep, masked, 0.0)
                weight = jnp.where(keep, weight, 0.0)
            top = jnp.maximum(top, masked)
            total = total + masked
            count = count + weight
    send_stats(out, top, total, count)


def first_stats(flat, devices):
    rows = flat.rows


    def body(points, text, south, rep, errors, mapped, target, out):
        for k in range(12):
            for r in range(rows):
                spread(text[k * rows + r : k * rows + r + 1], rep, k, flat.at(r, -2), flat.span)
            spread(south[k * rows : k * rows + 1], rep, k, flat.at(rows, -2), flat.span)
        own_stats(flat, points, rep, errors, mapped, target, flat.own_blocks(), out)

    t = flat.tiles
    return call(
        body,
        [(12, t, LANES), (4, t, LANES), (12, t, LANES), (12, t, LANES), (devices, 1, LANES)],
        in_vmem=(0, 1, 2),
    )


def outer_values(flat, points, rep, errors, mapped, target, far, first_row, second_row):
    rows, cols, span = flat.rows, flat.cols, flat.span
    down, up, maps = row_message(flat)
    for n in range(3 * COMPS):
        points[COMPS + n, run_of(flat, -2, 0, cols - 1)] = far[n * cols : (n + 1) * cols]

    def unpack(south, north):
        for source, runs, first in ((north, down, -2), (south, up, rows)):
            for n, r, c0, c1, at in runs:
                points[n, run_of(flat, r, c0, c1)] = source[at : at + c1 - c0 + 1]
            for k in range(12):
                for j in range(2):
                    row = maps + 2 * k + j
                    spread(source[row : row + 1], rep, k, flat.at(first + j, -2), span)

    by_parity("row", unpack, first_row, second_row)
    own = set(flat.own_blocks())
    inner = set(f for f in own if f + SUB <= flat.at(rows - 1, -2))
    for f in flat.blocks(-2, -2, rows, flat.cols + 1):
        if f not in inner:
            outer = f + SUB <= flat.at(-1, -2)
            known = f in own and f + SUB <= flat.at(rows, -2)
            for d in range(1 if outer or known else 0, 4):
                link_values(flat, f, d, points, rep, errors, mapped, target)


def weigh(blocks, points, errors, weights, scale):
    for f in blocks:
        for d in range(4):
            weights[d, f : f + SUB] = points[d * COMPS + 6, f : f + SUB] * scale / (scale + errors[d, f : f + SUB])


def tile_sums(flat, f, points, mapped, target, weights):
    gram = {}
    cross = {}

    def put(store, key, value):
        store[key] = value if key not in store else store[key] + value

    for d in range(4):
        for end in range(2):
            at = f if end == 0 else f - flat.shift[d]
            rows = slice(at, at + SUB)
            base = d * COMPS + 3 * end
            x = [points[base + c, rows] for c in range(3)]
            other = target if end == 0 else mapped
            weight = weights[d, rows]
            weighted = [weight * v for v in x] + [weight]
            for a, b in GRAM:
                if a == 3:
                    put(gram, (a, b), weighted[b])
                else:
                    put(gram, (a, b), weighted[a] * x[b])
            for c in range(3):
                scaled = weight * other[3 * d + c, rows]
                put(cross, (c, 3), scaled)
                for b in range(3):
                    put(cross, (c, b), scaled * x[b])
    return gram, cross


def solve_small(gram, cross):
    factor = {}
    inverse = {}
    for a in range(4):
        for b in range(a + 1):
            value = gram[a, b]
            for i in range(b):
                value = value - factor[a, i] * factor[b, i]
            if a == b:
                inverse[a] = 1.0 / jnp.sqrt(value)
            else:
                factor[a, b] = value * inverse[b]
    result = []
    for c in range(3):
        forward = []
        for a in range(4):
            value = cross[c, a]
            for i in range(a):
                value = value - factor[a, i] * forward[i]
            forward.append(value * inverse[a])
        backward = [None] * 4
        for a in (3, 2, 1, 0):
            value = forward[a]
            for i in range(a + 1, 4):
                value = value - factor[i, a] * backward[i]
            backward[a] = value * inverse[a]
        result.extend(backward)
    return result


def update(flat, blocks, points, rep, mapped, target, weights, damping):
    group = iota((SUB, LANES), 1) // SUB
    results = []
    for start in range(0, len(blocks), LANES // SUB):
        part = blocks[start : start + LANES // SUB]
        gram, cross, old = {}, {}, {}
        for b, f in enumerate(part):
            keep = group == b

            def place(store, key, value):
                store[key] = value if b == 0 else jnp.where(keep, value, store[key])

            sums = tile_sums(flat, f, points, mapped, target, weights)
            for store, found in zip((gram, cross), sums):
                for key, value in found.items():
                    place(store, key, jnp.broadcast_to(jnp.sum(value, axis=1, keepdims=True), value.shape))
            for k in range(12):
                place(old, (k // 4, k % 4), rep[k, f : f + SUB])
        for a in range(4):
            gram[a, a] = gram[a, a] + damping
        for key, value in old.items():
            cross[key] = cross[key] + damping * value
        results.append((part, solve_small(gram, cross)))
    return results


def replicate(results, out):
    for part, solved in results:
        for k, value in enumerate(solved):
            for b, f in enumerate(part):
                out[k, f : f + SUB] = jnp.broadcast_to(value[:, b * SUB : b * SUB + 1], (SUB, LANES))


def first_update(flat, devices):
    rows, cols = flat.rows, flat.cols

    def body(*refs):
        got, far, first_row, second_row = refs[5:9]
        points, rep, errors, mapped, target, new_rep, out, weights = refs[9:]
        state = (points, rep, errors, mapped, target)
        outer_values(flat, *state, far, first_row, second_row)
        largest, mean_error = read_stats(got)
        scale = 0.25 * largest + 1e-06
        damping = damping_scale * mean_error + 1.0
        weigh(flat.blocks(-2, -2, rows, cols + 1), points, errors, weights, scale)
        blocks = flat.blocks(-1, -1, rows, cols)
        replicate(update(flat, blocks, points, rep, mapped, target, weights, damping), new_rep)
        blocks = flat.blocks(-1, -1, rows - 1, cols)
        own_stats(flat, points, new_rep, errors, mapped, target, blocks, out)

    t = flat.tiles
    return call(
        body,
        [(4 * COMPS, t, LANES)] + [(n, t, LANES) for n in (12, 4, 12, 12, 12)] + [(devices, 1, LANES)],
        [(4, t, LANES)],
        in_vmem=range(9),
        aliases={i: i for i in range(5)},
    )


def take_lanes(lines, at, count):
    pieces = []
    while count:
        n, lane = divmod(at, LANES)
        size = min(count, LANES - lane)
        pieces.append(lines[n][:, lane : lane + size])
        at, count = at + size, count - size
    return pieces[0] if len(pieces) == 1 else jnp.concatenate(pieces, axis=1)


def last_update(flat):
    rows, cols = flat.rows, flat.cols

    def body(got0, got1, points, rep, errors, mapped, target, aligned, stats, weights):
        first, mean0 = read_stats(got0)
        largest, mean_error = read_stats(got1)
        scale = 0.25 * largest + 1e-06
        damping = damping_scale * mean_error + 1.0
        weigh(flat.blocks(-1, -1, rows - 1, cols), points, errors, weights, scale)
        results = update(flat, flat.own_blocks(), points, rep, mapped, target, weights, damping)
        diagonal = iota((SUB, LANES), 0) == lax.rem(iota((SUB, LANES), 1), SUB)
        for k in range(12):
            lines = []
            for part, solved in results:
                lines.append(jnp.sum(jnp.where(diagonal, solved[k], 0.0), axis=0, keepdims=True))
            for r in range(rows):
                at = flat.at(r, 0) - results[0][0][0]
                aligned[k, r : r + 1] = take_lanes(lines, at, cols)
        row = iota((2, 2), 0)
        col = iota((2, 2), 1)
        first, largest, mean0, mean_error = [v[0:2, 0:2] for v in (first, largest, mean0, mean_error)]
        stats[...] = jnp.where(row == 0, jnp.where(col == 0, first, largest), jnp.where(col == 0, mean0, mean_error))

    t = flat.tiles
    return call(body, [(12, rows, cols), (2, 2)], [(4, t, LANES)], in_vmem=range(7), results=None)


def onward(array, axis, by):
    peers = lax.axis_size(axis)
    return lax.ppermute(array, axis, [(i, i + by) for i in range(peers) if 0 <= i + by < peers])


def everyone(array):
    return lax.all_to_all(array, ("row", "col"), 0, 0)


def on_device(points_here, points_there, outlier_mask, transforms):
    rows, cols = transforms.shape[2:]
    devices = lax.axis_size("row") * lax.axis_size("col")
    flat = Flat(rows, cols)
    points, padded, to_first, to_second, to_far = pack_cols(flat)(
        points_here, points_there, outlier_mask, transforms.reshape(12 * rows, cols)
    )
    first_swap = swap(to_first, "col", 0)
    second_swap = swap(to_second, "col", 1)
    below = onward(padded, "row", -1)
    far = onward(to_far, "row", 1)
    points, text, to_first, to_second = pack_rows(flat)(points, padded, first_swap, second_swap)
    first_row = swap(to_first, "row", 0)
    second_row = swap(to_second, "row", 1)
    rep, errors, mapped, target, sent = first_stats(flat, devices)(points, text, below)
    got0 = everyone(sent)
    points, _, errors, mapped, target, rep, sent = first_update(flat, devices)(
        points, rep, errors, mapped, target, got0, far, first_row, second_row
    )
    got1 = everyone(sent)
    aligned, stats = last_update(flat)(got0, got1, points, rep, errors, mapped, target)
    return aligned.reshape(3, 4, rows, cols), stats


def solution(mesh):
    return jax.shard_map(
        on_device,
        mesh=mesh,
        in_specs=(
            P(None, None, "row", "col", None),
            P(None, None, "row", "col", None),
            P(None, "row", "col", None),
            P(None, None, "row", "col"),
        ),
        out_specs=(P(None, None, "row", "col"), P()),
        check_vma=False,
    )
```
